512 devices in a mesh: batch: 64 (over x, z, y_hi), space: 8 (over y_lo, core).
Axes of the slice: x: 4, y: 8 (y_hi: 2, y_lo: 4; y = y_hi * 4 + y_lo), z: 8, core: 2. Of those that a mesh axis runs over, the one named last changes fastest.
Arguments:
- latents: float32 [64, 32, 64, 4], P('batch', 'space'), may hold values from -16 to 16
- noise_draw: float32 [64, 32, 64, 4], P('batch', 'space'), may hold values from -5 to 5
- timesteps: int32 [64], P('batch'), may hold values from 200 to 799
- inlet_conv: bfloat16 [36, 320], replicated, may hold values from -1 to 1
- time_first: bfloat16 [320, 1280], P(None, 'batch'), may hold values from -0.3125 to 0.3125
- time_first_bias: float32 [1280], replicated, may hold values from -4 to 4
- time_second: bfloat16 [1280, 320], P(None, 'batch'), may hold values from -0.3125 to 0.3125
- time_second_bias: float32 [320], replicated, may hold values from -4 to 4
- conv_first: bfloat16 [2880, 320], P(None, 'batch'), may hold values from -0.109375 to 0.109375
- conv_second: bfloat16 [2880, 320], P(None, 'batch'), may hold values from -0.109375 to 0.109375
- proj_inner: bfloat16 [320, 320], P(None, 'batch'), may hold values from -0.3125 to 0.3125
- query_weight: bfloat16 [320, 320], P(None, 'batch'), may hold values from -30 to 30
- key_weight: bfloat16 [320, 320], P(None, 'batch'), may hold values from -1 to 1
- value_weight: bfloat16 [320, 320], P(None, 'batch'), may hold values from -0.625 to 0.625
- attn_out: bfloat16 [320, 320], P(None, 'batch'), may hold values from -0.625 to 0.625
- proj_outer: bfloat16 [320, 320], P(None, 'batch'), may hold values from -0.3125 to 0.3125
- outlet_conv: bfloat16 [2880, 4], replicated, may hold values from -0.109375 to 0.109375
- first_gain: float32 [320], replicated, may hold values from 0.1 to 1.9
- second_gain: float32 [320], replicated, may hold values from 0.1 to 1.9
- third_gain: float32 [320], replicated, may hold values from 0.1 to 1.9
- final_gain: float32 [320], replicated, may hold values from 0.1 to 1.9
- layer_gain: float32 [320], replicated, may hold values from 0.1 to 1.9
Outputs:
- guidance: float32 [64, 32, 64, 4], P('batch', 'space')
The draws below stay inside these ranges and needn't reach their ends.
All inputs are finite; a program needn't handle non-finite values.
Results may differ from the reference program's by a relative error of at most 0.029.
Values may be sent and summed in bfloat16 or wider, within the bound.
A program may use at most 64 MiB of HBM per device.

```python
import math
import jax
import jax.numpy as jnp
from jax import lax

C = 320
TEMB = 1280
HEADS = 8
HEAD_SIZE = 40
GROUPS = 32
LAT = 4
H = 32
W = 64
STEPS = 1000
VIEWS = 64


def draw_latents(key, part):
    shape = (VIEWS, H, W, LAT)
    ramp = jnp.exp(jnp.linspace(0.0, math.log(4.0), H, dtype=jnp.float32))[None, :, None, None]
    field = jax.random.truncated_normal(jax.random.fold_in(key, 7), -4.0, 4.0, shape, jnp.float32) * ramp
    return jnp.clip(field, -16.0, 16.0)


def attention_pair(key):
    shape = (C, C)
    key_part = jax.random.truncated_normal(jax.random.fold_in(key, 11), -6.0, 6.0, shape, jnp.float32) / math.sqrt(C)
    free_part = jax.random.truncated_normal(jax.random.fold_in(key, 12), -6.0, 6.0, shape, jnp.float32) / math.sqrt(C)
    query_part = 2.5 * free_part
    return (jnp.clip(query_part, -30.0, 30.0), jnp.clip(key_part, -1.0, 1.0))


def draw_query_weight(key, part):
    return attention_pair(key)[0].astype(jnp.bfloat16)


def draw_key_weight(key, part):
    return attention_pair(key)[1].astype(jnp.bfloat16)


def touch_ends(array, own_key, smallest, high):
    place = [jax.random.randint(jax.random.fold_in(own_key, axis), (), 0, length) for axis, length in enumerate(array.shape)]
    main_axis = array.shape.index(max(array.shape))
    beside = place[:main_axis] + [(place[main_axis] + 1) % array.shape[main_axis]] + place[main_axis + 1:]
    return array.at[tuple(place)].set(smallest).at[tuple(beside)].set(high)


def level_of(stream_key, dims, pieces, smallest, high):
    def one(axis_at, parts):
        heights = jax.random.uniform(jax.random.fold_in(jax.random.fold_in(stream_key, 6), axis_at), (parts,), jnp.float32, smallest / len(pieces), high / len(pieces))
        return jnp.repeat(jnp.exp(heights), dims[axis_at] // parts).reshape((-1,) + (1,) * (len(dims) - axis_at - 1))

    loudness = one(*pieces[0])
    for cut in pieces[1:]:
        loudness = loudness * one(*cut)
    return loudness


def scatter_about(key, extent, width, limit, pieces=(), kind=jnp.bfloat16):
    drawn = jax.random.normal(key, extent, jnp.float32) * width
    if len(pieces) > 0:
        drawn = level_of(key, extent, pieces, -0.22, 0.18) * drawn
    return jnp.clip(drawn, min=-limit, max=limit).astype(kind)


def setup_inputs(seed: int = 0) -> dict:
    streams_of = jax.random.split(jax.random.key(seed), 23)
    latents = draw_latents(jax.random.fold_in(streams_of[22], 71), 0)
    noise_draw = scatter_about(streams_of[1], (VIEWS, H, W, LAT), 1.0, 5.0, ((0, 64), (1, 8)), jnp.float32)
    timesteps = touch_ends(jax.random.randint(streams_of[2], (VIEWS,), 200, 800), jax.random.fold_in(streams_of[2], 1), 200, 799).astype(jnp.int32)
    inlet_conv = scatter_about(streams_of[3], (9 * LAT, C), (9 * LAT) ** -0.5, 1.0)
    time_first = scatter_about(streams_of[4], (C, TEMB), C ** -0.5, 0.3125, ((1, 64),))
    time_first_bias = scatter_about(streams_of[5], (TEMB,), 1.0, 4.0, (), jnp.float32)
    time_second = scatter_about(streams_of[6], (TEMB, C), (TEMB // 4) ** -0.5, 0.3125, ((1, 64),))
    time_second_bias = scatter_about(streams_of[7], (C,), 1.0, 4.0, (), jnp.float32)
    conv_first = scatter_about(streams_of[8], (9 * C, C), (9 * C) ** -0.5, 0.109375, ((1, 64),))
    conv_second = scatter_about(streams_of[9], (9 * C, C), (9 * C) ** -0.5, 0.109375, ((1, 64),))
    proj_inner = scatter_about(streams_of[10], (C, C), C ** -0.5, 0.3125, ((1, 64),))
    query_weight = draw_query_weight(jax.random.fold_in(streams_of[22], 71), 0)
    key_weight = draw_key_weight(jax.random.fold_in(streams_of[22], 71), 0)
    value_weight = scatter_about(streams_of[13], (C, C), (C // 4) ** -0.5, 0.625, ((1, 64),))
    attn_out = scatter_about(streams_of[14], (C, C), (C // 4) ** -0.5, 0.625, ((1, 64),))
    proj_outer = scatter_about(streams_of[15], (C, C), C ** -0.5, 0.3125, ((1, 64),))
    outlet_conv = scatter_about(streams_of[16], (9 * C, LAT), (9 * C) ** -0.5, 0.109375)
    first_gain = jnp.clip(1.0 + 0.18 * jax.random.normal(streams_of[17], (C,), jnp.float32), 0.1, 1.9)
    second_gain = jnp.clip(1.0 + 0.18 * jax.random.normal(streams_of[18], (C,), jnp.float32), 0.1, 1.9)
    third_gain = jnp.clip(1.0 + 0.18 * jax.random.normal(streams_of[19], (C,), jnp.float32), 0.1, 1.9)
    final_gain = jnp.clip(1.0 + 0.18 * jax.random.normal(streams_of[20], (C,), jnp.float32), 0.1, 1.9)
    layer_gain = jnp.clip(1.0 + 0.18 * jax.random.normal(streams_of[21], (C,), jnp.float32), 0.1, 1.9)
    return {"latents": latents, "noise_draw": noise_draw, "timesteps": timesteps, "inlet_conv": inlet_conv, "time_first": time_first, "time_first_bias": time_first_bias, "time_second": time_second, "time_second_bias": time_second_bias, "conv_first": conv_first, "conv_second": conv_second, "proj_inner": proj_inner, "query_weight": query_weight, "key_weight": key_weight, "value_weight": value_weight, "attn_out": attn_out, "proj_outer": proj_outer, "outlet_conv": outlet_conv, "first_gain": first_gain, "second_gain": second_gain, "third_gain": third_gain, "final_gain": final_gain, "layer_gain": layer_gain}


EPS_GROUP = 1e-06
EPS_BLOCK = 1e-05
EPS_LAYER = 1e-05

def plan():
    fraction = jnp.arange(STEPS, dtype=jnp.float32) / (STEPS - 1)
    beta_root = math.sqrt(0.00085) + fraction * (math.sqrt(0.012) - math.sqrt(0.00085))
    return jnp.cumprod(1.0 - beta_root * beta_root)

def lookup(timesteps):
    plan_tab = plan()
    matches = jnp.arange(STEPS, dtype=jnp.int32)[None, :] == timesteps[:, None]
    return lax.optimization_barrier(jnp.sum(jnp.where(matches, plan_tab[None, :], 0.0), axis=1))

def time_embed(timesteps, first, first_bias, second, second_bias):
    halfway = first.shape[0] // 2
    frequency = jnp.exp(-math.log(10000.0) * jnp.arange(halfway, dtype=jnp.float32) / halfway)
    angles = timesteps.astype(jnp.float32)[:, None] * frequency[None, :]
    waveform = jnp.concatenate([jnp.cos(angles), jnp.sin(angles)], axis=1).astype(jnp.bfloat16)
    inner = jax.nn.silu(jnp.dot(waveform, first, preferred_element_type=jnp.float32) + first_bias)
    hidden = jax.nn.silu(inner).astype(jnp.bfloat16)
    return jnp.dot(hidden, second, preferred_element_type=jnp.float32) + second_bias

def convolve(field, kernel):
    height, breadth, width_in = field.shape
    padded = jnp.pad(field, ((1, 1), (1, 1), (0, 0)))
    result = jnp.zeros((height, breadth, kernel.shape[1]), jnp.float32)
    for offset in range(9):
        row_off, col_off = (offset // 3, offset % 3)
        window = padded[row_off:row_off + height, col_off:col_off + breadth, :].astype(jnp.float32)
        taps = kernel[offset * width_in:(offset + 1) * width_in].astype(jnp.float32)
        result = result + jnp.einsum('hwc,cd->hwd', window, taps)
    return result

def group_norm(field, gain_vec, epsilon):
    height, breadth, chan_n = field.shape
    grouped = field.reshape(height, breadth, GROUPS, chan_n // GROUPS)
    number = height * breadth * (chan_n // GROUPS)
    means = lax.optimization_barrier(jnp.sum(grouped, axis=(0, 1, 3))) / number
    squares = lax.optimization_barrier(jnp.sum(grouped * grouped, axis=(0, 1, 3))) / number
    factor = lax.rsqrt(squares - means * means + epsilon)
    normal_f = (grouped - means[:, None]) * factor[:, None]
    return normal_f.reshape(height, breadth, chan_n) * gain_vec

def layer_norm(field, gain_vec):
    means = lax.optimization_barrier(jnp.mean(field, axis=-1, keepdims=True))
    centred = field - means
    spread = lax.optimization_barrier(jnp.mean(centred * centred, axis=-1, keepdims=True))
    return centred * lax.rsqrt(spread + EPS_LAYER) * gain_vec

def attend(queries, key_rows, value_rows):
    token_n = queries.shape[0]
    factor = 1.0 / math.sqrt(HEAD_SIZE)

    def arrange(field):
        return field.reshape(token_n, HEADS, HEAD_SIZE).transpose(1, 0, 2)

    def one_head(items):
        query_one, key_one, value_one = items
        scores = jnp.dot(query_one, key_one.T, preferred_element_type=jnp.float32) * factor
        row_max = lax.optimization_barrier(jnp.max(scores, axis=1, keepdims=True))
        weights = jnp.exp(scores - row_max)
        row_sum = lax.optimization_barrier(jnp.sum(weights, axis=1, keepdims=True))
        return jnp.dot(weights.astype(jnp.bfloat16), value_one, preferred_element_type=jnp.float32) / row_sum
    outputs = lax.map(one_head, (arrange(queries), arrange(key_rows), arrange(value_rows)))
    return outputs.transpose(1, 0, 2).reshape(token_n, HEADS * HEAD_SIZE).astype(jnp.bfloat16)

def reference(latents, noise_draw, timesteps, inlet_conv, time_first, time_first_bias, time_second, time_second_bias, conv_first, conv_second, proj_inner, query_weight, key_weight, value_weight, attn_out, proj_outer, outlet_conv, first_gain, second_gain, third_gain, final_gain, layer_gain):
    abar_all = lookup(timesteps)
    embed_all = time_embed(timesteps, time_first, time_first_bias, time_second, time_second_bias)

    def one_view(items):
        latent_one, noise_one, embed_one, abar = items
        noisy = (jnp.sqrt(abar) * latent_one + jnp.sqrt(1.0 - abar) * noise_one).astype(jnp.bfloat16)
        opening = convolve(noisy, inlet_conv).astype(jnp.bfloat16)
        active = jax.nn.silu(group_norm(opening.astype(jnp.float32), first_gain, EPS_BLOCK)).astype(jnp.bfloat16)
        middle = (convolve(active, conv_first) + embed_one).astype(jnp.bfloat16)
        active = jax.nn.silu(group_norm(middle.astype(jnp.float32), second_gain, EPS_BLOCK)).astype(jnp.bfloat16)
        block_one = (opening.astype(jnp.float32) + convolve(active, conv_second)).astype(jnp.bfloat16)
        normed = group_norm(block_one.astype(jnp.float32), third_gain, EPS_GROUP).astype(jnp.bfloat16)
        height, breadth, chan_n = normed.shape
        flattened = normed.reshape(height * breadth, chan_n)
        projected = jnp.dot(flattened, proj_inner, preferred_element_type=jnp.float32)
        tokens_in = layer_norm(projected, layer_gain).astype(jnp.bfloat16)
        queries = jnp.dot(tokens_in, query_weight, preferred_element_type=jnp.float32).astype(jnp.bfloat16)
        key_rows = jnp.dot(tokens_in, key_weight, preferred_element_type=jnp.float32).astype(jnp.bfloat16)
        value_rows = jnp.dot(tokens_in, value_weight, preferred_element_type=jnp.float32).astype(jnp.bfloat16)
        attended = attend(queries, key_rows, value_rows)
        mixture = (jnp.dot(attended, attn_out, preferred_element_type=jnp.float32) + projected).astype(jnp.bfloat16)
        outer = jnp.dot(mixture, proj_outer, preferred_element_type=jnp.float32).reshape(height, breadth, chan_n)
        block_two = (block_one.astype(jnp.float32) + outer).astype(jnp.bfloat16)
        active = jax.nn.silu(group_norm(block_two.astype(jnp.float32), final_gain, EPS_BLOCK)).astype(jnp.bfloat16)
        predicted = convolve(active, outlet_conv)
        return (1.0 - abar) * (predicted - noise_one)
    return lax.map(one_view, (latents, noise_draw, embed_all, abar_all))
```

```python
import math

import jax
import jax.numpy as jnp
from jax import lax
from jax.sharding import PartitionSpec as P
from jax.experimental import pallas as pl
from jax.experimental.pallas import tpu as pltpu

HEADS = 8
HEAD_SIZE = 40
GROUPS = 32
STEPS = 1000


EPS_GROUP = 1e-06
EPS_BLOCK = 1e-05
EPS_LAYER = 1e-05


def laid_out(parts, dim):
    parts = jnp.moveaxis(parts, 0, dim)
    shape = parts.shape
    return parts.reshape(*shape[:dim], shape[dim] * shape[dim + 1], *shape[dim + 2 :])


def from_everyone(shard, axis):
    length = lax.axis_size(axis)
    return lax.all_to_all(
        jnp.broadcast_to(shard[None], (length, *shard.shape)), axis, 0, 0, tiled=True
    )


def collect(shard, axis, dim):
    return laid_out(from_everyone(shard, axis), dim)


def extended(cells, sides, width):
    for axis, dim in sides:
        count = lax.axis_size(axis)
        ends = count - 1
        head = lax.slice_in_dim(cells, 0, width, axis=dim)
        tail = lax.slice_in_dim(cells, cells.shape[dim] - width, cells.shape[dim], axis=dim)
        cells = jnp.concatenate(
            [
                lax.ppermute(tail, axis, [(i, (i + 1) % count) for i in range(ends)]),
                cells,
                lax.ppermute(head, axis, [((i + 1) % count, i) for i in range(ends)]),
            ],
            axis=dim,
        )
    return cells


def of_everyone(shard, axis):
    everything = from_everyone(shard, axis)
    return jnp.sum(everything, axis=0)


def packed_total(arrays, axis):
    vector, at, gathered = (jnp.concatenate([a.reshape(-1) for a in arrays]), 0, [])
    running = of_everyone(vector, axis)
    for a in arrays:
        gathered.append(running[at : at + a.size].reshape(a.shape))
        at += a.size
    return tuple(gathered)


def in_one_piece(arrays, axis, dim, along):
    widths = [a.shape[along] for a in arrays]
    both = jnp.concatenate(arrays, axis=along)
    filled = lax.all_gather(both, axis, axis=dim, tiled=True)
    return tuple(jnp.split(filled, [sum(widths[:k]) for k in range(1, len(widths))], axis=along))


def turned_gather(arrays, axis, dims):
    turned = [jnp.moveaxis(a, dim, 0) for a, dim in zip(arrays, dims)]
    widths = [t[0].size for t in turned]
    both = jnp.concatenate([t.reshape(-1, w) for t, w in zip(turned, widths)], axis=1)
    filled = lax.all_gather(both, axis, axis=0, tiled=True)
    parts = jnp.split(filled, [sum(widths[:k]) for k in range(1, len(widths))], axis=1)
    return tuple(
        (
            jnp.moveaxis(b.reshape(-1, *t.shape[1:]), 0, dim)
            for b, t, dim in zip(parts, turned, dims)
        )
    )


def plan():
    fraction = jnp.arange(STEPS, dtype=jnp.float32) / (STEPS - 1)
    beta_root = math.sqrt(0.00085) + fraction * (math.sqrt(0.012) - math.sqrt(0.00085))
    return jnp.cumprod(1.0 - beta_root * beta_root)


def lookup(timesteps):
    plan_tab = plan()
    matches = jnp.arange(STEPS, dtype=jnp.int32)[None, :] == timesteps[:, None]
    return jnp.sum(jnp.where(matches, plan_tab[None, :], 0.0), axis=1)


def waveform_of(timesteps, halfway):
    frequency = jnp.exp(-math.log(10000.0) * jnp.arange(halfway, dtype=jnp.float32) / halfway)
    angles = timesteps.astype(jnp.float32)[:, None] * frequency[None, :]
    return jnp.concatenate([jnp.cos(angles), jnp.sin(angles)], axis=1).astype(jnp.bfloat16)


def embed_sharded(timesteps, first, first_bias, second, second_bias):
    all_steps = collect(timesteps, "batch", 0)
    position = lax.axis_index("batch")
    width_one = first.shape[1]
    width_two = second.shape[1]
    waveform = waveform_of(all_steps, first.shape[0] // 2)
    bias_one = lax.dynamic_slice_in_dim(first_bias, position * width_one, width_one, 0)
    inner = jax.nn.silu(jnp.dot(waveform, first, preferred_element_type=jnp.float32) + bias_one)
    hidden = jax.nn.silu(inner).astype(jnp.bfloat16)
    hidden_all = collect(hidden, "batch", 1)
    bias_two = lax.dynamic_slice_in_dim(second_bias, position * width_two, width_two, 0)
    columns = jnp.dot(hidden_all, second, preferred_element_type=jnp.float32) + bias_two
    return lax.all_to_all(columns, "batch", split_axis=0, concat_axis=1, tiled=True)


CHUNKS = 8
CHUNK = 1408
OWN = CHUNKS // 2
MESH = pl.DeviceIdType.MESH


def widened(turned, width):
    return jnp.pad(turned, ((0, 0), (0, width - turned.shape[1])))


def piece_of(first, second, convs, squares):
    tf = first.T.reshape(4, 5, 320).transpose(1, 0, 2)
    tf = jnp.pad(tf, ((0, 0), (0, 0), (0, 64))).reshape(5, 1536)
    ts = second.T.reshape(5, 64, 4, 5).transpose(0, 2, 1, 3).reshape(5, 4, 320)
    ts = jnp.pad(ts, ((0, 0), (0, 0), (0, 64))).reshape(5, 1536)
    rows = [tf, ts] + [widened(c.T, 2944) for c in convs] + [widened(m.T, 384) for m in squares]
    rows = jnp.concatenate(rows, axis=1)
    rows = jnp.pad(rows, ((0, 3), (0, 0)))
    return rows.reshape(8, CHUNKS, CHUNK).transpose(1, 0, 2)


def gather_kernel(piece, w, y_s, y_r, z_s, z_r, x_s, x_r, c_s, c_r):
    b = lax.axis_index("batch")
    s = lax.axis_index("space")
    yh = lax.rem(b, 2)
    z = lax.rem(lax.div(b, 2), 8)
    x = lax.div(b, 16)
    core = lax.rem(s, 2)
    sib = s + 1 - 2 * core
    mate = b + 1 - 2 * yh

    def at_z(zz):
        return (x * 8 + zz) * 2 + yh

    def at_x(xx):
        return (xx * 8 + z) * 2 + yh

    zs = [lax.rem(z + d, 8) for d in range(8)]
    xs = [lax.rem(x + d, 4) for d in range(4)]
    z_from = [lax.rem(z + 8 - d, 8) for d in range(8)]
    x_from = [lax.rem(x + 4 - d, 4) for d in range(4)]

    barrier = pltpu.get_barrier_semaphore()
    for dev in [(mate, s), (b, sib)] + [(at_z(q), s) for q in zs[1:]] + [(at_x(q), s) for q in xs[1:]]:
        pl.semaphore_signal(barrier, inc=1, device_id=dev, device_id_type=MESH)
    for i in range(OWN):
        w[2 * i + core, b] = piece[2 * i + core]
    pl.semaphore_wait(barrier, 12)

    def send(src, dst, ss, rs, dev):
        return pltpu.make_async_remote_copy(
            src_ref=src, dst_ref=dst, send_sem=ss, recv_sem=rs, device_id=dev, device_id_type=MESH
        )

    ys, zc, xc, cc = [], {}, {}, {}
    for i in range(OWN):
        c = 2 * i + core
        copy = send(piece.at[c], w.at[c, b], y_s.at[i], y_r.at[i], (mate, s))
        copy.start()
        ys.append(copy)
    pair = b - yh
    for i in range(OWN):
        c = 2 * i + core
        ys[i].wait_recv()
        for d in range(1, 8):
            part = w.at[c, pl.ds(pair, 2)]
            copy = send(part, part, z_s.at[i, d - 1], z_r.at[i, d - 1], (at_z(zs[d]), s))
            copy.start()
            zc[i, d] = copy
    for i in range(OWN):
        c = 2 * i + core
        for d in range(1, 8):
            zc[i, d].wait_recv()
        block = w.at[c, pl.ds(x * 16, 16)]
        for d in range(1, 4):
            copy = send(block, block, x_s.at[i, d - 1], x_r.at[i, d - 1], (at_x(xs[d]), s))
            copy.start()
            xc[i, d] = copy
        copy = send(block, block, c_s.at[i, 0], c_r.at[i, 0], (b, sib))
        copy.start()
        cc[i, 0] = copy
    for i in range(OWN):
        c = 2 * i + core
        for d in range(1, 4):
            xc[i, d].wait_recv()
            block = w.at[c, pl.ds(x_from[d] * 16, 16)]
            copy = send(block, block, c_s.at[i, d], c_r.at[i, d], (b, sib))
            copy.start()
            cc[i, d] = copy
    for i in range(OWN):
        for d in range(4):
            cc[i, d].wait_recv()
    for i in range(OWN):
        ys[i].wait_send()
        for d in range(1, 8):
            zc[i, d].wait_send()
        for d in range(1, 4):
            xc[i, d].wait_send()
        for d in range(4):
            cc[i, d].wait_send()


def gather_weights(piece):
    dma = pltpu.SemaphoreType.DMA
    return pl.pallas_call(
        gather_kernel,
        out_shape=jax.ShapeDtypeStruct((CHUNKS, 64, 8, CHUNK), jnp.bfloat16),
        in_specs=[pl.BlockSpec(memory_space=pltpu.VMEM)],
        out_specs=pl.BlockSpec(memory_space=pltpu.VMEM),
        scratch_shapes=[
            dma((OWN,)),
            dma((OWN,)),
            dma((OWN, 7)),
            dma((OWN, 7)),
            dma((OWN, 3)),
            dma((OWN, 3)),
            dma((OWN, 4)),
            dma((OWN, 4)),
        ],
        compiler_params=pltpu.CompilerParams(collective_id=0, has_side_effects=True, vmem_limit_bytes=40 << 20),
        name="gather_weights",
    )(piece)


def embed_local(timesteps, tf, first_bias, ts, second_bias):
    wave = waveform_of(timesteps, 160)
    inner = jnp.einsum("vk,bjik->vbij", wave, tf, preferred_element_type=jnp.float32)
    inner = jax.nn.silu(inner.reshape(1, 1280) + first_bias)
    hidden = jax.nn.silu(inner).astype(jnp.bfloat16)
    hidden = hidden.reshape(1, 64, 4, 5).transpose(0, 2, 1, 3).reshape(1, 4, 320)
    return jnp.einsum("vik,nik->vn", hidden, ts, preferred_element_type=jnp.float32) + second_bias


def convolve(padded, kernel):
    height = padded.shape[1] - 2
    breadth = padded.shape[2] - 2
    width_in = padded.shape[3]
    result = None
    for offset in range(9):
        row_off, col_off = (offset // 3, offset % 3)
        window = padded[:, row_off : row_off + height, col_off : col_off + breadth, :]
        partial_sum = jnp.einsum(
            "bhwc,cd->bhwd",
            window,
            kernel[offset * width_in : (offset + 1) * width_in],
            preferred_element_type=jnp.float32,
        )
        result = partial_sum if result is None else result + partial_sum
    return result


def with_rims(field):
    padded = extended(field, (("space", 1),), 1)
    return jnp.pad(padded, ((0, 0), (0, 0), (1, 1), (0, 0)))


def with_latent_rims(field):
    padded = extended(field, (("space", 1),), 1)
    return jnp.pad(padded, ((0, 0), (0, 0), (1, 1), (0, 0)))


def group_norm(field, gain_vec, epsilon):
    view_n, height, breadth, chan_n = field.shape
    grouped = field.reshape(view_n, height, breadth, GROUPS, chan_n // GROUPS)
    sums_local = jnp.sum(grouped, axis=(1, 2, 4))
    squares_local = jnp.sum(grouped * grouped, axis=(1, 2, 4))
    sums_all, squares_all = packed_total((sums_local, squares_local), "space")
    number = height * lax.axis_size("space") * breadth * (chan_n // GROUPS)
    means = sums_all / number
    squares = squares_all / number
    factor = lax.rsqrt(squares - means * means + epsilon)
    normal_f = (grouped - means[:, None, None, :, None]) * factor[:, None, None, :, None]
    return normal_f.reshape(view_n, height, breadth, chan_n) * gain_vec


def layer_norm(field, gain_vec):
    means = jnp.mean(field, axis=-1, keepdims=True)
    centred = field - means
    spread = jnp.mean(centred * centred, axis=-1, keepdims=True)
    return centred * lax.rsqrt(spread + EPS_LAYER) * gain_vec


def keys_everywhere(queries, key_rows, value_rows):
    view_n, token_n, chan_n = queries.shape
    factor = 1.0 / math.sqrt(HEAD_SIZE)
    query_heads = queries.reshape(view_n, token_n, HEADS, HEAD_SIZE)
    row_max = jnp.full((view_n, HEADS, token_n), -jnp.inf, jnp.float32)
    row_sum = jnp.zeros((view_n, HEADS, token_n), jnp.float32)
    accum = jnp.zeros((view_n, HEADS, token_n, HEAD_SIZE), jnp.float32)
    key_part, value_part = in_one_piece((key_rows, value_rows), "space", 1, 0)
    length = key_part.shape[1]
    block_n = min(512, length)
    for offset in range(0, length, block_n):
        key_blk = key_part[:, offset : offset + block_n]
        value_blk = value_part[:, offset : offset + block_n]
        rows_here = key_blk.shape[1]
        key_blk = key_blk.reshape(view_n, rows_here, HEADS, HEAD_SIZE)
        value_blk = value_blk.reshape(view_n, rows_here, HEADS, HEAD_SIZE)
        scores = (
            jnp.einsum("bqhd,bkhd->bhqk", query_heads, key_blk, preferred_element_type=jnp.float32)
            * factor
        )
        new_max = jnp.maximum(row_max, jnp.max(scores, axis=-1))
        shrink = jnp.exp(row_max - new_max)
        weights = jnp.exp(scores - new_max[..., None])
        row_sum = row_sum * shrink + jnp.sum(weights, axis=-1)
        accum = accum * shrink[..., None] + jnp.einsum(
            "bhqk,bkhd->bhqd",
            weights.astype(jnp.bfloat16),
            value_blk,
            preferred_element_type=jnp.float32,
        )
        row_max = new_max
    row_max, row_sum, accum = (row_max, row_sum, accum)
    result = accum / row_sum[..., None]
    return result.transpose(0, 2, 1, 3).reshape(view_n, token_n, chan_n).astype(jnp.bfloat16)


def project(field, matrix):
    return jnp.einsum("btc,cd->btd", field, matrix, preferred_element_type=jnp.float32)


def body(
    latents,
    noise_draw,
    timesteps,
    inlet_conv,
    time_first,
    time_first_bias,
    time_second,
    time_second_bias,
    conv_first,
    conv_second,
    proj_inner,
    query_weight,
    key_weight,
    value_weight,
    attn_out,
    proj_outer,
    outlet_conv,
    first_gain,
    second_gain,
    third_gain,
    final_gain,
    layer_gain,
):
    piece = piece_of(
        time_first,
        time_second,
        (conv_first, conv_second),
        (proj_inner, query_weight, key_weight, value_weight, attn_out, proj_outer),
    )
    whole = gather_weights(piece)
    whole = whole.transpose(1, 2, 0, 3).reshape(64, 8, CHUNKS * CHUNK)[:, :5]
    tf = whole[:, :, :1536].reshape(64, 5, 4, 384)[..., :320]
    whole = whole.reshape(320, CHUNKS * CHUNK)
    ts = whole[:, 1536:3072].reshape(320, 4, 384)[..., :320]
    conv_one = whole[:, 3072 : 3072 + 2880].T
    conv_two = whole[:, 6016 : 6016 + 2880].T
    inner_w, query_w, key_w, value_w, output_w, outer_w = (
        whole[:, 8960 + 384 * i : 8960 + 384 * i + 320].T for i in range(6)
    )
    embedded = embed_local(timesteps, tf, time_first_bias, ts, time_second_bias)
    alpha_bar = lookup(timesteps)[:, None, None, None]
    noisy = (jnp.sqrt(alpha_bar) * latents + jnp.sqrt(1.0 - alpha_bar) * noise_draw).astype(
        jnp.bfloat16
    )
    opening = convolve(with_latent_rims(noisy), inlet_conv).astype(jnp.bfloat16)
    active = jax.nn.silu(group_norm(opening.astype(jnp.float32), first_gain, EPS_BLOCK)).astype(
        jnp.bfloat16
    )
    middle = (convolve(with_rims(active), conv_one) + embedded[:, None, None, :]).astype(
        jnp.bfloat16
    )
    active = jax.nn.silu(group_norm(middle.astype(jnp.float32), second_gain, EPS_BLOCK)).astype(
        jnp.bfloat16
    )
    block_one = (opening.astype(jnp.float32) + convolve(with_rims(active), conv_two)).astype(
        jnp.bfloat16
    )
    normed = group_norm(block_one.astype(jnp.float32), third_gain, EPS_GROUP).astype(jnp.bfloat16)
    view_n, height, breadth, chan_n = normed.shape
    flattened = normed.reshape(view_n, height * breadth, chan_n)
    projected = project(flattened, inner_w)
    tokens_in = layer_norm(projected, layer_gain).astype(jnp.bfloat16)
    queries = project(tokens_in, query_w).astype(jnp.bfloat16)
    key_rows = project(tokens_in, key_w).astype(jnp.bfloat16)
    value_rows = project(tokens_in, value_w).astype(jnp.bfloat16)
    attended = keys_everywhere(queries, key_rows, value_rows)
    mixture = (project(attended, output_w) + projected).astype(jnp.bfloat16)
    outer = project(mixture, outer_w).reshape(view_n, height, breadth, chan_n)
    block_two = (block_one.astype(jnp.float32) + outer).astype(jnp.bfloat16)
    active = jax.nn.silu(group_norm(block_two.astype(jnp.float32), final_gain, EPS_BLOCK)).astype(
        jnp.bfloat16
    )
    predicted = convolve(with_rims(active), outlet_conv)
    return (1.0 - alpha_bar) * (predicted - noise_draw)


def solution(mesh):
    in_specs = (
        P("batch", "space", None, None),
        P("batch", "space", None, None),
        P("batch"),
        P(),
        P(None, "batch"),
        P(),
        P(None, "batch"),
        P(),
        P(None, "batch"),
        P(None, "batch"),
        P(None, "batch"),
        P(None, "batch"),
        P(None, "batch"),
        P(None, "batch"),
        P(None, "batch"),
        P(None, "batch"),
        P(),
        P(),
        P(),
        P(),
        P(),
        P(),
    )
    out_specs = P("batch", "space", None, None)
    return jax.shard_map(body, mesh=mesh, in_specs=in_specs, out_specs=out_specs, check_vma=False)
```

```python
import math

import jax
import jax.numpy as jnp
from jax import lax
from jax.experimental import pallas as pl
from jax.experimental.pallas import tpu as pltpu
from jax.sharding import PartitionSpec as P

HEADS = 8
HEAD_SIZE = 40
GROUPS = 32
STEPS = 1000


EPS_GROUP = 1e-06
EPS_BLOCK = 1e-05
EPS_LAYER = 1e-05


def plan():
    fraction = jnp.arange(STEPS, dtype=jnp.float32) / (STEPS - 1)
    beta_root = math.sqrt(0.00085) + fraction * (math.sqrt(0.012) - math.sqrt(0.00085))
    return jnp.cumprod(1.0 - beta_root * beta_root)


def lookup(timesteps):
    plan_tab = plan()
    matches = jnp.arange(STEPS, dtype=jnp.int32)[None, :] == timesteps[:, None]
    return jnp.sum(jnp.where(matches, plan_tab[None, :], 0.0), axis=1)


def waveform_of(timesteps, halfway):
    frequency = jnp.exp(-math.log(10000.0) * jnp.arange(halfway, dtype=jnp.float32) / halfway)
    angles = timesteps.astype(jnp.float32)[:, None] * frequency[None, :]
    return jnp.concatenate([jnp.cos(angles), jnp.sin(angles)], axis=1).astype(jnp.bfloat16)


C = 320
WIDE = 512
ROW = 64
OWN_TOKENS = 256
EDGED = OWN_TOKENS + 2 * ROW
TAPS = 2944
CHUNKS = 8
CHUNK = 1408
OWN = CHUNKS // 2
AT_FIRST = 0
AT_SECOND = 1536
AT_CONV_ONE = 3072
AT_CONV_TWO = 6016
AT_INNER, AT_QUERY, AT_KEY, AT_VALUE, AT_MIX, AT_OUTER = (8960 + 384 * i for i in range(6))
MESH = pl.DeviceIdType.MESH
F32 = jnp.float32
BF16 = jnp.bfloat16


def widened(turned, width):
    return jnp.pad(turned, ((0, 0), (0, width - turned.shape[1])))


def piece_of(first, second, convs, squares):
    tf = first.T.reshape(4, 5, C).transpose(1, 0, 2)
    tf = jnp.pad(tf, ((0, 0), (0, 0), (0, 64))).reshape(5, 1536)
    ts = second.T.reshape(5, 64, 4, 5).transpose(0, 2, 1, 3).reshape(5, 4, C)
    ts = jnp.pad(ts, ((0, 0), (0, 0), (0, 64))).reshape(5, 1536)
    rows = [tf, ts] + [widened(c.T, TAPS) for c in convs] + [widened(m.T, 384) for m in squares]
    rows = jnp.concatenate(rows, axis=1)
    rows = jnp.pad(rows, ((0, 3), (0, 0)))
    return rows.reshape(8, CHUNKS, CHUNK).transpose(1, 0, 2)


def mm(a, b):
    return lax.dot_general(a, b, (((1,), (0,)), ((), ())), preferred_element_type=F32)


def mt(a, b):
    return lax.dot_general(a, b, (((1,), (1,)), ((), ())), preferred_element_type=F32)


def exactly(product, v, matrix):
    high = v.astype(BF16)
    rest = v - high.astype(F32)
    mid = rest.astype(BF16)
    low = (rest - mid.astype(F32)).astype(BF16)
    return product(high, matrix) + product(mid, matrix) + product(low, matrix)


def silu(v):
    half = 0.5 * v
    return half + half * jnp.tanh(half)


def block_kernel(
    piece,
    nt,
    wave,
    vecs,
    win,
    wout,
    out,
    w,
    wn,
    taps,
    xt,
    nview,
    start,
    mid6,
    two6,
    block,
    nat,
    stats,
    spread,
    gwide,
    gslim,
    keys,
    values,
    query,
    base,
    y_s,
    y_r,
    z_s,
    z_r,
    x_s,
    x_r,
    c_s,
    c_r,
    n_s,
    n_r,
    t_s,
    t_r,
    h_s,
    h_r,
    up_s,
    up_r,
    dn_s,
    dn_r,
    k_s,
    k_r,
):
    b = lax.axis_index("batch")
    s = lax.axis_index("space")
    yh = lax.rem(b, 2)
    z = lax.rem(lax.div(b, 2), 8)
    x = lax.div(b, 16)
    core = lax.rem(s, 2)
    chip = lax.div(s, 2)
    sib = s + 1 - 2 * core
    mate = b + 1 - 2 * yh

    def at_z(zz):
        return (x * 8 + zz) * 2 + yh

    def at_x(xx):
        return (xx * 8 + z) * 2 + yh

    zs = [lax.rem(z + d, 8) for d in range(8)]
    xs = [lax.rem(x + d, 4) for d in range(4)]
    x_from = [lax.rem(x + 4 - d, 4) for d in range(4)]
    peers = [lax.rem(s + d, 8) for d in range(8)]
    peers_from = [lax.rem(s + 8 - d, 8) for d in range(8)]

    barrier = pltpu.get_barrier_semaphore()
    friends = [(mate, s)] + [(at_z(q), s) for q in zs[1:]] + [(at_x(q), s) for q in xs[1:]]
    friends += [(b, q) for q in peers[1:]]
    for dev in friends:
        pl.semaphore_signal(barrier, inc=1, device_id=dev, device_id_type=MESH)
    for i in range(OWN):
        w[2 * i + core, b] = piece[2 * i + core]
    nview[s] = nt[...]
    pl.semaphore_wait(barrier, len(friends))

    def send(src, dst, ss, rs, dev):
        return pltpu.make_async_remote_copy(
            src_ref=src, dst_ref=dst, send_sem=ss, recv_sem=rs, device_id=dev, device_id_type=MESH
        )

    pending = []
    ys, zc, xc, cc = [], {}, {}, {}
    for i in range(OWN):
        c = 2 * i + core
        copy = send(piece.at[c], w.at[c, b], y_s.at[i], y_r.at[i], (mate, s))
        copy.start()
        ys.append(copy)
        pending.append(copy)
    ns = []
    for d in range(1, 8):
        copy = send(nt, nview.at[s], n_s.at[d - 1], n_r.at[d - 1], (b, peers[d]))
        copy.start()
        ns.append(copy)
        pending.append(copy)

    wide_i = lax.broadcasted_iota(jnp.int32, (WIDE, C), 0)
    slim_j = lax.broadcasted_iota(jnp.int32, (WIDE, C), 1)
    hit = (lax.shift_right_logical(wide_i, 3) * 5 + lax.bitwise_and(wide_i, 7) == slim_j) & (
        lax.bitwise_and(wide_i, 7) < 5
    )
    spread[...] = jnp.where(hit, 1.0, 0.0).astype(BF16)
    gi = lax.broadcasted_iota(jnp.int32, (WIDE, WIDE), 0)
    gj = lax.broadcasted_iota(jnp.int32, (WIDE, WIDE), 1)
    same = lax.shift_right_logical(gi, 4) == lax.shift_right_logical(gj, 4)
    gwide[...] = jnp.where(same, 1.0, 0.0).astype(BF16)
    ni = lax.broadcasted_iota(jnp.int32, (C, C), 0)
    nj = lax.broadcasted_iota(jnp.int32, (C, C), 1)
    apart = ni - lax.div(nj, 10) * 10
    gslim[...] = jnp.where((apart >= 0) & (apart < 10), 1.0, 0.0).astype(BF16)
    wide_vecs = exactly(mt, vecs[...], spread[...])
    win_wide = mt(win[...], spread[...]).astype(BF16)

    for copy in ns:
        copy.wait_recv()
    field = jnp.concatenate([nview[q] for q in range(8)], axis=1).astype(F32)
    token = lax.broadcasted_iota(jnp.int32, (16, 2048), 1)
    above = jnp.where(token < ROW, 0.0, pltpu.roll(field, ROW, 1))
    below = jnp.where(token >= 2048 - ROW, 0.0, pltpu.roll(field, 2048 - ROW, 1))
    rows = jnp.concatenate([above, field, below, jnp.zeros((80, 2048), F32)], axis=0)
    xt[0:ROW, :] = jnp.zeros((ROW, 128), BF16)
    xt[ROW + 2048 : 2 * ROW + 2048, :] = jnp.zeros((ROW, 128), BF16)
    xt[ROW : ROW + 2048, :] = rows.T.astype(BF16)

    pair = b - yh
    for i in range(OWN):
        c = 2 * i + core
        ys[i].wait_recv()
        for d in range(1, 8):
            part = w.at[c, pl.ds(pair, 2)]
            copy = send(part, part, z_s.at[i, d - 1], z_r.at[i, d - 1], (at_z(zs[d]), s))
            copy.start()
            zc[i, d] = copy
            pending.append(copy)

    def start_sums(q, carry):
        total, squared = carry
        part = mm(xt[pl.ds(pl.multiple_of(ROW + q * 256, 64), 256), :], win_wide)
        part = part.astype(BF16).astype(F32)
        return total + jnp.sum(part, axis=0, keepdims=True), squared + jnp.sum(part * part, axis=0, keepdims=True)

    zero = jnp.zeros((1, WIDE), F32)
    total, squared = lax.fori_loop(0, 8, start_sums, (zero, zero))
    start[...] = mm(xt[pl.ds(pl.multiple_of(s * 256, 256), EDGED), :], win_wide).astype(BF16)

    def stacked(total, squared):
        width = total.shape[1]
        return jnp.concatenate([total, squared, jnp.zeros((6, width), F32)], axis=0)

    def affine(sums, groups, gain, epsilon):
        sums = exactly(mm, sums, groups) * (1.0 / 20480.0)
        mean = sums[0:1]
        factor = lax.rsqrt(sums[1:2] - mean * mean + epsilon) * gain
        return factor, -mean * factor

    line = lax.broadcasted_iota(jnp.int32, (EDGED, 1), 0)
    outside = ((s == 0) & (line < ROW)) | ((s == 7) & (line >= EDGED - ROW))
    column = lax.bitwise_and(line, ROW - 1)

    def into_taps(field, factor, shift):
        active = jnp.where(outside, 0.0, silu(field.astype(F32) * factor + shift)).astype(BF16)
        slim = mm(active, spread[...])
        west = jnp.where(column == 0, 0.0, pltpu.roll(slim, 1, 0)).astype(BF16)
        east = jnp.where(column == ROW - 1, 0.0, pltpu.roll(slim, EDGED - 1, 0)).astype(BF16)
        for dx, shifted in enumerate((west, slim.astype(BF16), east)):
            for dy in range(3):
                tap = 3 * dy + dx
                taps[:, tap * C : (tap + 1) * C] = shifted[dy * ROW : dy * ROW + OWN_TOKENS]

    for i in range(OWN):
        c = 2 * i + core
        for d in range(1, 8):
            zc[i, d].wait_recv()
        part = w.at[c, pl.ds(x * 16, 16)]
        for d in range(1, 4):
            copy = send(part, part, x_s.at[i, d - 1], x_r.at[i, d - 1], (at_x(xs[d]), s))
            copy.start()
            xc[i, d] = copy
            pending.append(copy)
        copy = send(part, part, c_s.at[i, 0], c_r.at[i, 0], (b, sib))
        copy.start()
        cc[i, 0] = copy
        pending.append(copy)

    taps[:, 9 * C :] = jnp.zeros((OWN_TOKENS, TAPS - 9 * C), BF16)
    factor, shift = affine(stacked(total, squared), gwide[...], wide_vecs[5:6], EPS_BLOCK)
    into_taps(start[...], factor, shift)

    def arrive(i):
        c = 2 * i + core
        for d in range(1, 4):
            xc[i, d].wait_recv()
            part = w.at[c, pl.ds(x_from[d] * 16, 16)]
            copy = send(part, part, c_s.at[i, d], c_r.at[i, d], (b, sib))
            copy.start()
            cc[i, d] = copy
            pending.append(copy)

    def unpack(i):
        for d in range(4):
            cc[i, d].wait_recv()

        def two(p, _):
            for c in (2 * i, 2 * i + 1):
                both = w[c, pl.ds(2 * p, 2)].astype(F32).reshape(16, CHUNK)
                wn[pl.ds(pl.multiple_of(p * 16, 16), 16), c * CHUNK : (c + 1) * CHUNK] = both.astype(BF16)
            return 0

        lax.fori_loop(0, 32, two, 0)

    arrive(0)
    arrive(1)
    unpack(0)
    unpack(1)
    embedded = wide_vecs[4:5]
    for i in range(4):
        inner = mt(wave[...], wn[:, AT_FIRST + 384 * i : AT_FIRST + 384 * i + C])
        hidden = silu(silu(inner + wide_vecs[i : i + 1])).astype(BF16)
        hidden = mm(hidden, spread[...]).astype(BF16)
        embedded = embedded + mt(hidden, wn[:, AT_SECOND + 384 * i : AT_SECOND + 384 * i + C])[0:1]
    arrive(2)
    unpack(2)
    middle = (mt(taps[...], wn[:, AT_CONV_ONE : AT_CONV_ONE + TAPS]) + embedded).astype(BF16)

    def exchange(layer, field, edged):
        edged[ROW : ROW + OWN_TOKENS, :] = field
        wide = field.astype(F32)
        stats[layer, s] = stacked(jnp.sum(wide, axis=0, keepdims=True), jnp.sum(wide * wide, axis=0, keepdims=True))
        up = send(
            edged.at[pl.ds(ROW, ROW)],
            edged.at[pl.ds(ROW + OWN_TOKENS, ROW)],
            h_s.at[layer, 0],
            h_r.at[layer, 0],
            (b, lax.rem(s + 7, 8)),
        )
        down = send(
            edged.at[pl.ds(OWN_TOKENS, ROW)],
            edged.at[pl.ds(0, ROW)],
            h_s.at[layer, 1],
            h_r.at[layer, 1],
            (b, lax.rem(s + 1, 8)),
        )

        @pl.when(s > 0)
        def _():
            up.start()

        @pl.when(s < 7)
        def _():
            down.start()

        copies = []
        for d in range(1, 8):
            copy = send(
                stats.at[layer, s], stats.at[layer, s], t_s.at[layer, d - 1], t_r.at[layer, d - 1], (b, peers[d])
            )
            copy.start()
            copies.append(copy)
            pending.append(copy)
        return up, down, copies

    def gather_stats(layer, copies):
        for copy in copies:
            copy.wait_recv()
        sums = stats[layer, 0]
        for q in range(1, 8):
            sums = sums + stats[layer, q]
        return sums

    def exchanged(layer, up, down, copies):
        @pl.when(s < 7)
        def _():
            up.wait_recv()

        @pl.when(s > 0)
        def _():
            down.wait_recv()

        @pl.when(s > 0)
        def _():
            up.wait_send()

        @pl.when(s < 7)
        def _():
            down.wait_send()

        return gather_stats(layer, copies)

    swap = exchange(0, middle, mid6)
    arrive(3)
    unpack(3)
    sums = exchanged(0, *swap)
    factor, shift = affine(sums, gwide[...], wide_vecs[6:7], EPS_BLOCK)
    into_taps(mid6[...], factor, shift)
    one = mt(taps[...], wn[:, AT_CONV_TWO : AT_CONV_TWO + TAPS])
    one = (one + start[ROW : ROW + OWN_TOKENS, :].astype(F32)).astype(BF16)
    block[...] = one

    slim = mm(one, spread[...])
    nat[s] = slim.astype(BF16)
    slim_sums = stacked(jnp.sum(slim, axis=0, keepdims=True), jnp.sum(slim * slim, axis=0, keepdims=True))
    stats[2, s] = jnp.concatenate([slim_sums, jnp.zeros((8, WIDE - C), F32)], axis=1)
    copies = []
    for d in range(1, 8):
        copy = send(stats.at[2, s], stats.at[2, s], t_s.at[2, d - 1], t_r.at[2, d - 1], (b, peers[d]))
        copy.start()
        copies.append(copy)
        pending.append(copy)

    def hop(source, towards, ss, rs):
        return send(nat.at[source], nat.at[source], ss, rs, (b, towards))

    def to_sib(source_chip):
        source = 2 * source_chip + core
        return hop(source, sib, k_s.at[source_chip], k_r.at[source_chip])

    first_up = hop(s, lax.rem(s + 2, 8), up_s.at[0], up_r.at[0])
    first_dn = hop(s, lax.rem(s + 6, 8), dn_s.at[0], dn_r.at[0])

    @pl.when(chip < 3)
    def _():
        first_up.start()

    @pl.when(chip > 0)
    def _():
        first_dn.start()

    to_sib(chip).start()

    def ups(h):
        source = s - 2 * h
        here = hop(source, lax.rem(s + 2, 8), up_s.at[min(h, 2)], up_r.at[h - 1])
        on = hop(source, lax.rem(s + 2, 8), up_s.at[min(h, 2)], up_r.at[min(h, 2)])
        return here, on

    def dns(h):
        source = s + 2 * h
        here = hop(source, lax.rem(s + 6, 8), dn_s.at[min(h, 2)], dn_r.at[h - 1])
        on = hop(source, lax.rem(s + 6, 8), dn_s.at[min(h, 2)], dn_r.at[min(h, 2)])
        return here, on

    for h in range(1, 4):

        @pl.when(chip >= h)
        def _(h=h):
            here, on = ups(h)
            here.wait_recv()
            if h < 3:

                @pl.when(chip < 3)
                def _():
                    on.start()

            to_sib(chip - h).start()

        @pl.when(chip + h <= 3)
        def _(h=h):
            here, on = dns(h)
            here.wait_recv()
            if h < 3:

                @pl.when(chip > 0)
                def _():
                    on.start()

            to_sib(chip + h).start()

    for q in range(4):
        source = 2 * q + 1 - core
        hop(source, sib, k_s.at[q], k_r.at[q]).wait_recv()
    sums = gather_stats(2, copies)
    factor, shift = affine(sums[:, :C], gslim[...], vecs[9:10, :], EPS_GROUP)
    lane = lax.broadcasted_iota(jnp.int32, (1, WIDE), 1)
    real = lax.bitwise_and(lane, 7) < 5

    def tokens(q):
        normed = (nat[q].astype(F32) * factor + shift).astype(BF16)
        projected = mt(normed, wn[:, AT_INNER : AT_INNER + C])
        mean = jnp.sum(projected, axis=1, keepdims=True) * (1.0 / C)
        centred = jnp.where(real, projected - mean, 0.0)
        spreadness = jnp.sum(centred * centred, axis=1, keepdims=True) * (1.0 / C)
        inside = (centred * lax.rsqrt(spreadness + EPS_LAYER) * wide_vecs[8:9]).astype(BF16)
        inside = mm(inside, spread[...]).astype(BF16)
        where = pl.ds(pl.multiple_of(q * 256, 256), 256)
        keys[where, :] = mt(inside, wn[:, AT_KEY : AT_KEY + C]).astype(BF16)
        values[where, :] = mt(inside, wn[:, AT_VALUE : AT_VALUE + C]).astype(BF16)
        return projected, inside

    projected, inside = tokens(s)
    base[...] = projected
    query[...] = mt(inside, wn[:, AT_QUERY : AT_QUERY + C]).astype(BF16)

    def others(d, _):
        tokens(lax.rem(s + d, 8))
        return 0

    lax.fori_loop(1, 8, others, 0)

    scale = math.log2(math.e) / math.sqrt(HEAD_SIZE)
    half = lax.broadcasted_iota(jnp.int32, (1, 128), 1) < 64

    def two_heads(p, _):
        lanes = pl.ds(pl.multiple_of(p * 128, 128), 128)
        mine = query[:, lanes]
        key_part = keys[:, lanes]
        value_part = values[:, lanes]
        results = []
        for keep in (half, jnp.logical_not(half)):
            one_query = jnp.where(keep, mine.astype(F32), 0.0).astype(BF16)
            scores = mt(one_query, key_part)
            top = jnp.max(scores, axis=1, keepdims=True)
            weights = jnp.exp2((scores - top) * scale)
            bottom = jnp.sum(weights, axis=1, keepdims=True)
            results.append(mm(weights.astype(BF16), value_part) / bottom)
        query[:, lanes] = jnp.where(half, results[0], results[1]).astype(BF16)
        return 0

    lax.fori_loop(0, 4, two_heads, 0)
    attended = mm(query[...], spread[...]).astype(BF16)
    mixture = (mt(attended, wn[:, AT_MIX : AT_MIX + C]) + base[...]).astype(BF16)
    mixture = mm(mixture, spread[...]).astype(BF16)
    outer = mt(mixture, wn[:, AT_OUTER : AT_OUTER + C])
    two = (block[...].astype(F32) + outer).astype(BF16)
    swap = exchange(1, two, two6)
    sums = exchanged(1, *swap)
    factor, shift = affine(sums, gwide[...], wide_vecs[7:8], EPS_BLOCK)
    into_taps(two6[...], factor, shift)
    out[...] = mt(taps[...], wout[...])

    for copy in pending:
        copy.wait_send()

    @pl.when(chip < 3)
    def _():
        first_up.wait_send()

    @pl.when(chip > 0)
    def _():
        first_dn.wait_send()

    for q in range(4):
        to_sib(q).wait_send()
    for h in range(1, 3):

        @pl.when((chip >= h) & (chip < 3))
        def _(h=h):
            ups(h)[1].wait_send()

        @pl.when((chip + h <= 3) & (chip > 0))
        def _(h=h):
            dns(h)[1].wait_send()


def run_block(piece, nt, wave, vecs, win, wout):
    dma = pltpu.SemaphoreType.DMA
    vmem = pl.BlockSpec(memory_space=pltpu.VMEM)
    return pl.pallas_call(
        block_kernel,
        out_shape=jax.ShapeDtypeStruct((OWN_TOKENS, 8), F32),
        in_specs=[vmem] * 6,
        out_specs=vmem,
        scratch_shapes=[
            pltpu.VMEM((CHUNKS, 64, 8, CHUNK), BF16),
            pltpu.VMEM((WIDE, CHUNKS * CHUNK), BF16),
            pltpu.VMEM((OWN_TOKENS, TAPS), BF16),
            pltpu.VMEM((2048 + 2 * ROW, 128), BF16),
            pltpu.VMEM((8, 16, OWN_TOKENS), BF16),
            pltpu.VMEM((EDGED, WIDE), BF16),
            pltpu.VMEM((EDGED, WIDE), BF16),
            pltpu.VMEM((EDGED, WIDE), BF16),
            pltpu.VMEM((OWN_TOKENS, WIDE), BF16),
            pltpu.VMEM((8, OWN_TOKENS, C), BF16),
            pltpu.VMEM((3, 8, 8, WIDE), F32),
            pltpu.VMEM((WIDE, C), BF16),
            pltpu.VMEM((WIDE, WIDE), BF16),
            pltpu.VMEM((C, C), BF16),
            pltpu.VMEM((2048, WIDE), BF16),
            pltpu.VMEM((2048, WIDE), BF16),
            pltpu.VMEM((OWN_TOKENS, WIDE), BF16),
            pltpu.VMEM((OWN_TOKENS, WIDE), F32),
            dma((OWN,)),
            dma((OWN,)),
            dma((OWN, 7)),
            dma((OWN, 7)),
            dma((OWN, 3)),
            dma((OWN, 3)),
            dma((OWN, 4)),
            dma((OWN, 4)),
            dma((7,)),
            dma((7,)),
            dma((3, 7)),
            dma((3, 7)),
            dma((2, 2)),
            dma((2, 2)),
            dma((3,)),
            dma((3,)),
            dma((3,)),
            dma((3,)),
            dma((4,)),
            dma((4,)),
        ],
        compiler_params=pltpu.CompilerParams(
            collective_id=0, has_side_effects=True, vmem_limit_bytes=58 << 20
        ),
        name="unet_level",
    )(piece, nt, wave, vecs, win, wout)


def body(
    latents,
    noise_draw,
    timesteps,
    inlet_conv,
    time_first,
    time_first_bias,
    time_second,
    time_second_bias,
    conv_first,
    conv_second,
    proj_inner,
    query_weight,
    key_weight,
    value_weight,
    attn_out,
    proj_outer,
    outlet_conv,
    first_gain,
    second_gain,
    third_gain,
    final_gain,
    layer_gain,
):
    piece = piece_of(
        time_first,
        time_second,
        (conv_first, conv_second),
        (proj_inner, query_weight, key_weight, value_weight, attn_out, proj_outer),
    )
    alpha_bar = lookup(timesteps)[:, None, None, None]
    noisy = (jnp.sqrt(alpha_bar) * latents + jnp.sqrt(1.0 - alpha_bar) * noise_draw).astype(BF16)
    padded = jnp.pad(noisy[0], ((0, 0), (1, 1), (0, 0)))
    turned = padded.transpose(2, 0, 1)
    nt = jnp.concatenate([turned[:, :, dx : dx + ROW] for dx in range(3)], axis=0).reshape(12, OWN_TOKENS)
    nt = jnp.pad(nt, ((0, 4), (0, 0)))
    wave = jnp.broadcast_to(waveform_of(timesteps, C // 2), (8, C))
    bias_one = time_first_bias.reshape(64, 4, 5).transpose(1, 0, 2).reshape(4, C)
    vecs = jnp.concatenate(
        [
            bias_one,
            jnp.stack([time_second_bias, first_gain, second_gain, final_gain, layer_gain, third_gain]),
            jnp.zeros((6, C), F32),
        ],
        axis=0,
    )
    win = jnp.pad(inlet_conv.reshape(3, 12, C), ((0, 0), (0, 4), (0, 0))).reshape(48, C)
    win = jnp.pad(win, ((0, 80), (0, 0)))
    wout = jnp.pad(outlet_conv.T, ((0, 4), (0, TAPS - 9 * C)))
    predicted = run_block(piece, nt, wave, vecs, win, wout)
    predicted = predicted[:, :4].reshape(noise_draw.shape)
    return (1.0 - alpha_bar) * (predicted - noise_draw)


def solution(mesh):
    in_specs = (
        P("batch", "space", None, None),
        P("batch", "space", None, None),
        P("batch"),
        P(),
        P(None, "batch"),
        P(),
        P(None, "batch"),
        P(),
        P(None, "batch"),
        P(None, "batch"),
        P(None, "batch"),
        P(None, "batch"),
        P(None, "batch"),
        P(None, "batch"),
        P(None, "batch"),
        P(None, "batch"),
        P(),
        P(),
        P(),
        P(),
        P(),
        P(),
    )
    out_specs = P("batch", "space", None, None)
    return jax.shard_map(body, mesh=mesh, in_specs=in_specs, out_specs=out_specs, check_vma=False)
```

```python
import math

import jax
import jax.numpy as jnp
from jax import lax
from jax.experimental import pallas as pl
from jax.experimental.pallas import tpu as pltpu
from jax.sharding import PartitionSpec as P

HEADS = 8
HEAD_SIZE = 40
GROUPS = 32
STEPS = 1000


EPS_GROUP = 1e-06
EPS_BLOCK = 1e-05
EPS_LAYER = 1e-05


C = 320
WIDE = 512
ROW = 64
OWN_TOKENS = 256
EDGED = OWN_TOKENS + 2 * ROW
TAPS = 2944
LENGTHS = (1408, 1408, 1280, 1280)
BASES = (0, 2816, 5632, 8192)
LANES = 10752
OWN = 4
AT_SECOND = 1280
AT_CONV_ONE = 2560
AT_CONV_TWO = 5504
AT_INNER, AT_QUERY, AT_KEY, AT_VALUE, AT_MIX, AT_OUTER = (8448 + 384 * i for i in range(6))
MESH = pl.DeviceIdType.MESH
F32 = jnp.float32
BF16 = jnp.bfloat16


def mm(a, b):
    return lax.dot_general(a, b, (((1,), (0,)), ((), ())), preferred_element_type=F32)


def mt(a, b):
    return lax.dot_general(a, b, (((1,), (1,)), ((), ())), preferred_element_type=F32)


def exactly(product, v, matrix):
    count = v.shape[0]
    high = v.astype(BF16).astype(F32)
    mid = (v - high).astype(BF16).astype(F32)
    low = v - high - mid
    parts = product(jnp.concatenate([high, mid, low], axis=0).astype(BF16), matrix)
    return parts[:count] + parts[count : 2 * count] + parts[2 * count :]


def silu(v):
    half = 0.5 * v
    return half + half * jnp.tanh(half)


def block_kernel(step, *refs):
    sources = refs[:21]
    out = refs[21]
    held = refs[22:43]
    (
        w0,
        w1,
        w2,
        w3,
        wn,
        flat,
        taps,
        xt,
        nt,
        nview,
        start,
        mid6,
        two6,
        block,
        nat,
        stats,
        spread,
        gwide,
        gslim,
        keys,
        values,
        query,
        base,
        l_s,
        y_s,
        y_r,
        a_s,
        a_r,
        b_s,
        b_r,
        c_s,
        c_r,
        n_s,
        n_r,
        t_s,
        t_r,
        h_s,
        h_r,
        up_s,
        up_r,
        dn_s,
        dn_r,
        k_s,
        k_r,
    ) = refs[43:]
    w = (w0, w1, w2, w3)
    b = lax.axis_index("batch")
    s = lax.axis_index("space")
    yh = lax.rem(b, 2)
    z = lax.rem(lax.div(b, 2), 8)
    x = lax.div(b, 16)
    core = lax.rem(s, 2)
    chip = lax.div(s, 2)
    sib = s + 1 - 2 * core
    mate = b + 1 - 2 * yh

    loads = [pltpu.make_async_copy(h, v, l_s.at[i]) for i, (h, v) in enumerate(zip(sources, held))]
    for load in loads:
        load.start()

    def at_z(d):
        return ((x * 8 + lax.rem(z + d, 8)) * 2 + yh, s)

    def at_x(d):
        return ((lax.rem(x + d, 4) * 8 + z) * 2 + yh, s)

    peers = [lax.rem(s + d, 8) for d in range(8)]
    barrier = pltpu.get_barrier_semaphore()
    friends = [(mate, 2 * q + core) for q in range(4)] + [at_z(1), at_z(7), at_x(1), at_x(3)]
    friends += [(b, q) for q in peers[1:]]
    for dev in friends:
        pl.semaphore_signal(barrier, inc=1, device_id=dev, device_id_type=MESH)
    for load in loads:
        load.wait()
    field8, wave, first, second, conv_a, conv_b = held[:6]
    squares = held[6:12]
    inlet, outlet, bias_a = held[12:15]
    third = held[20]

    def eight(rows):
        rows = rows.astype(F32)
        return jnp.concatenate([rows, jnp.zeros((8 - rows.shape[0], rows.shape[1]), F32)], axis=0).astype(BF16)

    flat[...] = jnp.zeros((8, LANES), BF16)
    turned = first[...].astype(F32)
    for i in range(4):
        flat[:, C * i : C * i + C] = eight(turned[5 * i : 5 * i + 5])
    flat[:, AT_SECOND : AT_SECOND + 1280] = eight(second[...])
    flat[:, AT_CONV_ONE : AT_CONV_ONE + 9 * C] = eight(conv_a[...])
    flat[:, AT_CONV_TWO : AT_CONV_TWO + 9 * C] = eight(conv_b[...])
    for i in range(6):
        flat[:, AT_INNER + 384 * i : AT_INNER + 384 * i + C] = eight(squares[i][...])

    place = lax.broadcasted_iota(jnp.int32, (8, 128), 0) * 128 + lax.broadcasted_iota(jnp.int32, (8, 128), 1)
    root = math.sqrt(0.00085) + place.astype(F32) / (STEPS - 1) * (math.sqrt(0.012) - math.sqrt(0.00085))
    abar = jnp.where(place <= step[0], 1.0 - root * root, 1.0)
    for shift in (1, 2, 4, 8, 16, 32, 64):
        abar = abar * pltpu.roll(abar, shift, 1)
    for shift in (1, 2, 4):
        abar = abar * pltpu.roll(abar, shift, 0)
    abar = abar[0:1, 0:1]
    noisy = jnp.sqrt(abar) * field8[0:4, :] + jnp.sqrt(1.0 - abar) * field8[4:8, :]
    noisy = noisy.astype(BF16).astype(F32)
    place = lax.bitwise_and(lax.broadcasted_iota(jnp.int32, (4, OWN_TOKENS), 1), ROW - 1)
    west = jnp.where(place == 0, 0.0, pltpu.roll(noisy, 1, 1))
    east = jnp.where(place == ROW - 1, 0.0, pltpu.roll(noisy, OWN_TOKENS - 1, 1))
    shifted = jnp.concatenate([west, noisy, east, jnp.zeros((4, OWN_TOKENS), F32)], axis=0).astype(BF16)
    nt[...] = shifted
    nview[s] = shifted
    own = [pl.ds(pl.multiple_of(BASES[i] + core * LENGTHS[i], 128), LENGTHS[i]) for i in range(OWN)]
    for i in range(OWN):
        w[i][core, x, z, yh] = flat[:, own[i]]
    pl.semaphore_wait(barrier, len(friends))

    def send(src, dst, ss, rs, dev):
        return pltpu.make_async_remote_copy(
            src_ref=src, dst_ref=dst, send_sem=ss, recv_sem=rs, device_id=dev, device_id_type=MESH
        )

    pending = []

    def go(copy):
        copy.start()
        pending.append(copy)
        return copy

    def crossing(i, k, to):
        return send(flat.at[:, own[i]], w[i].at[core, x, z, yh], y_s.at[i, k], y_r.at[i], (mate, 2 * to + core))

    for i in range(OWN):
        for k in range(2):

            @pl.when(chip == 0)
            def _(i=i, k=k):
                crossing(i, k, 3 - k).start()

            @pl.when(chip == 3)
            def _(i=i, k=k):
                crossing(i, k, k).start()

    ns = []
    for d in range(1, 8):
        ns.append(go(send(nt, nview.at[s], n_s.at[d - 1], n_r.at[d - 1], (b, peers[d]))))

    def z_ring(i, view, half):
        def block(d):
            return view(lax.rem(z + 8 + d, 8))

        def copies(t):
            if t < 3:
                one, two = block(-t), block(t)
            else:
                one, two = half(lax.rem(z + 8 - t, 8), 0), half(lax.rem(z + t, 8), 1)
            return (
                send(one, one, a_s.at[i, 2 * t], a_r.at[i, 2 * t], at_z(1)),
                send(two, two, a_s.at[i, 2 * t + 1], a_r.at[i, 2 * t + 1], at_z(7)),
            )

        def landed(t):
            if t < 3:
                return block(-1 - t), block(1 + t)
            return half(lax.rem(z + 4, 8), 0), half(lax.rem(z + 4, 8), 1)

        return 4, copies, landed

    def x_ring(i, view, half):
        def block(d):
            return view(lax.rem(x + 4 + d, 4))

        def copies(t):
            if t < 1:
                one, two = block(0), block(0)
            else:
                one, two = half(lax.rem(x + 3, 4), 0), half(lax.rem(x + 1, 4), 1)
            return (
                send(one, one, b_s.at[i, 2 * t], b_r.at[i, 2 * t], at_x(1)),
                send(two, two, b_s.at[i, 2 * t + 1], b_r.at[i, 2 * t + 1], at_x(3)),
            )

        def landed(t):
            if t < 1:
                return block(-1), block(1)
            return half(lax.rem(x + 2, 4), 0), half(lax.rem(x + 2, 4), 1)

        return 2, copies, landed

    def rings(i, k):
        wk = w[i].at[k]
        if i % 2 == 0:
            small = z_ring(i, lambda q: wk.at[x, q], lambda q, h: wk.at[x, q, h])
            large = x_ring(i, lambda q: wk.at[q], lambda q, h: wk.at[q, pl.ds(4 * h, 4)])
            mine = wk.at[x]
        else:
            small = x_ring(i, lambda q: wk.at[q, z], lambda q, h: wk.at[q, z, h])
            large = z_ring(i, lambda q: wk.at[:, q], lambda q, h: wk.at[pl.ds(2 * h, 2), q])
            mine = wk.at[:, z]
        return small, large, mine

    mine_rings = [rings(i, core) for i in range(OWN)]
    theirs = [rings(i, 1 - core) for i in range(OWN)]
    flying = {}

    def launch(i, which, t):
        flying[i, which, t] = [go(copy) for copy in mine_rings[i][which][1](t)]

    def to_sib(i, j, ref):
        go(send(ref, ref, c_s.at[i, j], c_r.at[i, j], (b, sib)))

    def land(i, which, t):
        count, _, landed = mine_rings[i][which]
        for copy in flying[i, which, t]:
            copy.wait_recv()
        if t + 1 < count:
            launch(i, which, t + 1)
        elif which == 0:
            launch(i, 1, 0)
            to_sib(i, 0, mine_rings[i][2])
        if which == 1:
            for j, ref in enumerate(landed(t)):
                to_sib(i, 1 + 2 * t + j, ref)

    def cross(i):
        send(flat.at[:, own[i]], w[i].at[core, x, z, 1 - yh], y_s.at[i, 0], y_r.at[i], (mate, s)).wait_recv()
        launch(i, 0, 0)

    def unpack(i):
        count, _, landed = theirs[i][1]
        refs = [theirs[i][2]] + [ref for t in range(count) for ref in landed(t)]
        for j, ref in enumerate(refs):
            send(ref, ref, c_s.at[i, j], c_r.at[i, j], (b, sib)).wait_recv()

        def two(p, _):
            for k in range(2):
                both = w[i][k, lax.div(p, 8), lax.rem(p, 8)].astype(F32).reshape(16, LENGTHS[i])
                at = BASES[i] + k * LENGTHS[i]
                wn[pl.ds(pl.multiple_of(p * 16, 16), 16), at : at + LENGTHS[i]] = both.astype(BF16)
            return 0

        lax.fori_loop(0, 32, two, 0)

    wide_i = lax.broadcasted_iota(jnp.int32, (WIDE, C), 0)
    slim_j = lax.broadcasted_iota(jnp.int32, (WIDE, C), 1)
    hit = (lax.shift_right_logical(wide_i, 3) * 5 + lax.bitwise_and(wide_i, 7) == slim_j) & (
        lax.bitwise_and(wide_i, 7) < 5
    )
    spread[...] = jnp.where(hit, 1.0, 0.0).astype(BF16)
    cross(0)
    cross(1)
    gi = lax.broadcasted_iota(jnp.int32, (WIDE, WIDE), 0)
    gj = lax.broadcasted_iota(jnp.int32, (WIDE, WIDE), 1)
    same = lax.shift_right_logical(gi, 4) == lax.shift_right_logical(gj, 4)
    gwide[...] = jnp.where(same, 1.0, 0.0).astype(BF16)
    ni = lax.broadcasted_iota(jnp.int32, (C, C), 0)
    nj = lax.broadcasted_iota(jnp.int32, (C, C), 1)
    apart = ni - lax.div(nj, 10) * 10
    gslim[...] = jnp.where((apart >= 0) & (apart < 10), 1.0, 0.0).astype(BF16)
    vecs = jnp.concatenate([v[...] for v in held[15:20]] + [jnp.zeros((3, C), F32)], axis=0)
    wide_vecs = exactly(mt, vecs, spread[...])
    taken = inlet[...].astype(F32)
    taken = [jnp.concatenate([taken[12 * q : 12 * q + 12], jnp.zeros((4, C), F32)], axis=0) for q in range(3)]
    win = jnp.concatenate(taken + [jnp.zeros((80, C), F32)], axis=0).astype(BF16)
    win_wide = mt(win, spread[...]).astype(BF16)
    land(1, 0, 0)
    land(0, 0, 0)

    for copy in ns:
        copy.wait_recv()
    field = jnp.concatenate([nview[q] for q in range(8)], axis=1).astype(F32)
    token = lax.broadcasted_iota(jnp.int32, (16, 2048), 1)
    above = jnp.where(token < ROW, 0.0, pltpu.roll(field, ROW, 1))
    below = jnp.where(token >= 2048 - ROW, 0.0, pltpu.roll(field, 2048 - ROW, 1))
    rows = jnp.concatenate([above, field, below, jnp.zeros((80, 2048), F32)], axis=0)
    xt[0:ROW, :] = jnp.zeros((ROW, 128), BF16)
    xt[ROW + 2048 : 2 * ROW + 2048, :] = jnp.zeros((ROW, 128), BF16)
    xt[ROW : ROW + 2048, :] = rows.T.astype(BF16)

    land(1, 0, 1)
    land(0, 0, 1)
    land(0, 0, 2)
    land(0, 0, 3)
    cross(2)
    cross(3)

    def start_sums(q, carry):
        total, squared = carry
        part = mm(xt[pl.ds(pl.multiple_of(ROW + q * 256, 64), 256), :], win_wide)
        part = part.astype(BF16).astype(F32)
        return total + jnp.sum(part, axis=0, keepdims=True), squared + jnp.sum(part * part, axis=0, keepdims=True)

    zero = jnp.zeros((1, WIDE), F32)
    total, squared = lax.fori_loop(0, 8, start_sums, (zero, zero))
    start[...] = mm(xt[pl.ds(pl.multiple_of(s * 256, 256), EDGED), :], win_wide).astype(BF16)

    def stacked(total, squared):
        width = total.shape[1]
        return jnp.concatenate([total, squared, jnp.zeros((6, width), F32)], axis=0)

    def affine(sums, groups, gain, epsilon):
        sums = exactly(mm, sums, groups) * (1.0 / 20480.0)
        mean = sums[0:1]
        factor = lax.rsqrt(sums[1:2] - mean * mean + epsilon) * gain
        return factor, -mean * factor

    line = lax.broadcasted_iota(jnp.int32, (EDGED, 1), 0)
    outside = ((s == 0) & (line < ROW)) | ((s == 7) & (line >= EDGED - ROW))
    column = lax.bitwise_and(line, ROW - 1)

    def into_taps(field, factor, shift):
        active = jnp.where(outside, 0.0, silu(field.astype(F32) * factor + shift)).astype(BF16)
        slim = mm(active, spread[...])
        west = jnp.where(column == 0, 0.0, pltpu.roll(slim, 1, 0)).astype(BF16)
        east = jnp.where(column == ROW - 1, 0.0, pltpu.roll(slim, EDGED - 1, 0)).astype(BF16)
        for dx, shifted in enumerate((west, slim.astype(BF16), east)):
            for dy in range(3):
                tap = 3 * dy + dx
                taps[:, tap * C : (tap + 1) * C] = shifted[dy * ROW : dy * ROW + OWN_TOKENS]

    land(1, 1, 0)
    land(2, 0, 0)
    land(3, 0, 0)
    taps[:, 9 * C :] = jnp.zeros((OWN_TOKENS, TAPS - 9 * C), BF16)
    factor, shift = affine(stacked(total, squared), gwide[...], wide_vecs[0:1], EPS_BLOCK)
    into_taps(start[...], factor, shift)

    land(1, 1, 1)
    land(0, 1, 0)
    land(2, 0, 1)
    land(3, 0, 1)
    row_p = lax.broadcasted_iota(jnp.int32, (C, 1), 0)
    target = 4 * row_p - 3 * lax.rem(row_p, 5)
    unit = lax.broadcasted_iota(jnp.int32, (C, 1280), 1)
    orders = [jnp.where(unit == target + 5 * i, 1.0, 0.0).astype(BF16) for i in range(4)]
    bias_rows = jnp.broadcast_to(bias_a[...], (8, 1280))
    biases = [exactly(mt, exactly(mt, bias_rows, orders[i]), spread[...]) for i in range(4)]
    land(2, 0, 2)
    land(1, 1, 2)
    land(0, 1, 1)
    unpack(0)
    land(2, 0, 3)
    land(1, 1, 3)
    unpack(1)
    waves = jnp.broadcast_to(wave[...], (8, C))
    hidden = jnp.zeros((8, 1280), F32)
    for i in range(4):
        blank = jnp.zeros((8, C), F32)
        placed = jnp.concatenate([waves, blank] if i % 2 == 0 else [blank, waves], axis=1).astype(BF16)
        first_at = 640 * (i // 2)
        inner = mt(placed, wn[:, first_at : first_at + 640])
        part = silu(silu(inner + biases[i])).astype(BF16)
        hidden = hidden + mm(mm(part, spread[...]).astype(BF16), orders[i])
    embedded = mt(hidden.astype(BF16), wn[:, AT_SECOND : AT_SECOND + 1280])[0:1] + wide_vecs[4:5]
    land(3, 1, 0)
    middle = (mt(taps[...], wn[:, AT_CONV_ONE : AT_CONV_ONE + TAPS]) + embedded).astype(BF16)

    def exchange(layer, field, edged):
        edged[ROW : ROW + OWN_TOKENS, :] = field
        wide = field.astype(F32)
        stats[layer, s] = stacked(jnp.sum(wide, axis=0, keepdims=True), jnp.sum(wide * wide, axis=0, keepdims=True))
        up = send(
            edged.at[pl.ds(ROW, ROW)],
            edged.at[pl.ds(ROW + OWN_TOKENS, ROW)],
            h_s.at[layer, 0],
            h_r.at[layer, 0],
            (b, lax.rem(s + 7, 8)),
        )
        down = send(
            edged.at[pl.ds(OWN_TOKENS, ROW)],
            edged.at[pl.ds(0, ROW)],
            h_s.at[layer, 1],
            h_r.at[layer, 1],
            (b, lax.rem(s + 1, 8)),
        )

        @pl.when(s > 0)
        def _():
            up.start()

        @pl.when(s < 7)
        def _():
            down.start()

        copies = []
        for d in range(1, 8):
            copy = send(
                stats.at[layer, s], stats.at[layer, s], t_s.at[layer, d - 1], t_r.at[layer, d - 1], (b, peers[d])
            )
            copy.start()
            copies.append(copy)
            pending.append(copy)
        return up, down, copies

    def gather_stats(layer, copies):
        for copy in copies:
            copy.wait_recv()
        sums = stats[layer, 0]
        for q in range(1, 8):
            sums = sums + stats[layer, q]
        return sums

    def exchanged(layer, up, down, copies):
        @pl.when(s < 7)
        def _():
            up.wait_recv()

        @pl.when(s > 0)
        def _():
            down.wait_recv()

        @pl.when(s > 0)
        def _():
            up.wait_send()

        @pl.when(s < 7)
        def _():
            down.wait_send()

        return gather_stats(layer, copies)

    swap = exchange(0, middle, mid6)
    land(2, 1, 0)
    land(3, 1, 1)
    sums = exchanged(0, *swap)
    factor, shift = affine(sums, gwide[...], wide_vecs[1:2], EPS_BLOCK)
    into_taps(mid6[...], factor, shift)
    land(3, 1, 2)
    land(2, 1, 1)
    unpack(2)
    land(3, 1, 3)
    unpack(3)
    one = mt(taps[...], wn[:, AT_CONV_TWO : AT_CONV_TWO + TAPS])
    one = (one + start[ROW : ROW + OWN_TOKENS, :].astype(F32)).astype(BF16)
    block[...] = one

    slim = mm(one, spread[...])
    nat[s] = slim.astype(BF16)
    slim_sums = stacked(jnp.sum(slim, axis=0, keepdims=True), jnp.sum(slim * slim, axis=0, keepdims=True))
    stats[2, s] = jnp.concatenate([slim_sums, jnp.zeros((8, WIDE - C), F32)], axis=1)
    copies = []
    for d in range(1, 8):
        copy = send(stats.at[2, s], stats.at[2, s], t_s.at[2, d - 1], t_r.at[2, d - 1], (b, peers[d]))
        copy.start()
        copies.append(copy)
        pending.append(copy)

    def hop(source, towards, ss, rs):
        return send(nat.at[source], nat.at[source], ss, rs, (b, towards))

    def kin(source_chip):
        source = 2 * source_chip + core
        return hop(source, sib, k_s.at[source_chip], k_r.at[source_chip])

    first_up = hop(s, lax.rem(s + 2, 8), up_s.at[0], up_r.at[0])
    first_dn = hop(s, lax.rem(s + 6, 8), dn_s.at[0], dn_r.at[0])

    @pl.when(chip < 3)
    def _():
        first_up.start()

    @pl.when(chip > 0)
    def _():
        first_dn.start()

    kin(chip).start()

    def ups(h):
        source = s - 2 * h
        here = hop(source, lax.rem(s + 2, 8), up_s.at[min(h, 2)], up_r.at[h - 1])
        on = hop(source, lax.rem(s + 2, 8), up_s.at[min(h, 2)], up_r.at[min(h, 2)])
        return here, on

    def dns(h):
        source = s + 2 * h
        here = hop(source, lax.rem(s + 6, 8), dn_s.at[min(h, 2)], dn_r.at[h - 1])
        on = hop(source, lax.rem(s + 6, 8), dn_s.at[min(h, 2)], dn_r.at[min(h, 2)])
        return here, on

    for h in range(1, 4):

        @pl.when(chip >= h)
        def _(h=h):
            here, on = ups(h)
            here.wait_recv()
            if h < 3:

                @pl.when(chip < 3)
                def _():
                    on.start()

            kin(chip - h).start()

        @pl.when(chip + h <= 3)
        def _(h=h):
            here, on = dns(h)
            here.wait_recv()
            if h < 3:

                @pl.when(chip > 0)
                def _():
                    on.start()

            kin(chip + h).start()

    for q in range(4):
        source = 2 * q + 1 - core
        hop(source, sib, k_s.at[q], k_r.at[q]).wait_recv()
    sums = gather_stats(2, copies)
    factor, shift = affine(sums[:, :C], gslim[...], third[...], EPS_GROUP)
    lane = lax.broadcasted_iota(jnp.int32, (1, WIDE), 1)
    real = lax.bitwise_and(lane, 7) < 5

    def tokens(q):
        normed = (nat[q].astype(F32) * factor + shift).astype(BF16)
        projected = mt(normed, wn[:, AT_INNER : AT_INNER + C])
        mean = jnp.sum(projected, axis=1, keepdims=True) * (1.0 / C)
        centred = jnp.where(real, projected - mean, 0.0)
        spreadness = jnp.sum(centred * centred, axis=1, keepdims=True) * (1.0 / C)
        inside = (centred * lax.rsqrt(spreadness + EPS_LAYER) * wide_vecs[3:4]).astype(BF16)
        inside = mm(inside, spread[...]).astype(BF16)
        where = pl.ds(pl.multiple_of(q * 256, 256), 256)
        keys[where, :] = mt(inside, wn[:, AT_KEY : AT_KEY + C]).astype(BF16)
        values[where, :] = mt(inside, wn[:, AT_VALUE : AT_VALUE + C]).astype(BF16)
        return projected, inside

    projected, inside = tokens(s)
    base[...] = projected
    query[...] = mt(inside, wn[:, AT_QUERY : AT_QUERY + C]).astype(BF16)

    def others(d, _):
        tokens(lax.rem(s + d, 8))
        return 0

    lax.fori_loop(1, 8, others, 0)

    scale = math.log2(math.e) / math.sqrt(HEAD_SIZE)
    half = lax.broadcasted_iota(jnp.int32, (1, 128), 1) < 64

    def two_heads(p, _):
        lanes = pl.ds(pl.multiple_of(p * 128, 128), 128)
        mine = query[:, lanes]
        key_part = keys[:, lanes]
        value_part = values[:, lanes]
        results = []
        for keep in (half, jnp.logical_not(half)):
            one_query = jnp.where(keep, mine.astype(F32), 0.0).astype(BF16)
            scores = mt(one_query, key_part)
            top = jnp.max(scores, axis=1, keepdims=True)
            weights = jnp.exp2((scores - top) * scale)
            bottom = jnp.sum(weights, axis=1, keepdims=True)
            results.append(mm(weights.astype(BF16), value_part) / bottom)
        query[:, lanes] = jnp.where(half, results[0], results[1]).astype(BF16)
        return 0

    lax.fori_loop(0, 4, two_heads, 0)
    attended = mm(query[...], spread[...]).astype(BF16)
    mixture = (mt(attended, wn[:, AT_MIX : AT_MIX + C]) + base[...]).astype(BF16)
    mixture = mm(mixture, spread[...]).astype(BF16)
    outer = mt(mixture, wn[:, AT_OUTER : AT_OUTER + C])
    two = (block[...].astype(F32) + outer).astype(BF16)
    swap = exchange(1, two, two6)
    sums = exchanged(1, *swap)
    factor, shift = affine(sums, gwide[...], wide_vecs[2:3], EPS_BLOCK)
    into_taps(two6[...], factor, shift)
    taken = outlet[...].astype(F32)
    taken = jnp.concatenate([taken, jnp.zeros((4, 9 * C), F32)], axis=0)
    taken = jnp.concatenate([taken, jnp.zeros((8, TAPS - 9 * C), F32)], axis=1).astype(BF16)
    predicted = mt(taken, taps[...])
    out[...] = (1.0 - abar) * (predicted[0:4] - field8[4:8, :])
    for i in range(OWN):
        for k in range(2):

            @pl.when(chip == 0)
            def _(i=i, k=k):
                crossing(i, k, 3 - k).wait_send()

            @pl.when(chip == 3)
            def _(i=i, k=k):
                crossing(i, k, k).wait_send()


    for copy in pending:
        copy.wait_send()

    @pl.when(chip < 3)
    def _():
        first_up.wait_send()

    @pl.when(chip > 0)
    def _():
        first_dn.wait_send()

    for q in range(4):
        kin(q).wait_send()
    for h in range(1, 3):

        @pl.when((chip >= h) & (chip < 3))
        def _(h=h):
            ups(h)[1].wait_send()

        @pl.when((chip + h <= 3) & (chip > 0))
        def _(h=h):
            dns(h)[1].wait_send()


def run_block(step, sources):
    dma = pltpu.SemaphoreType.DMA
    hbm = pl.BlockSpec(memory_space=pltpu.HBM)
    return pl.pallas_call(
        block_kernel,
        out_shape=jax.ShapeDtypeStruct((4, OWN_TOKENS), F32),
        in_specs=[pl.BlockSpec(memory_space=pltpu.SMEM)] + [hbm] * len(sources),
        out_specs=pl.BlockSpec(memory_space=pltpu.VMEM),
        scratch_shapes=[pltpu.VMEM(a.shape, a.dtype) for a in sources]
        + [pltpu.VMEM((2, 4, 8, 2, 8, length), BF16) for length in LENGTHS]
        + [
            pltpu.VMEM((WIDE, LANES), BF16),
            pltpu.VMEM((8, LANES), BF16),
            pltpu.VMEM((OWN_TOKENS, TAPS), BF16),
            pltpu.VMEM((2048 + 2 * ROW, 128), BF16),
            pltpu.VMEM((16, OWN_TOKENS), BF16),
            pltpu.VMEM((8, 16, OWN_TOKENS), BF16),
            pltpu.VMEM((EDGED, WIDE), BF16),
            pltpu.VMEM((EDGED, WIDE), BF16),
            pltpu.VMEM((EDGED, WIDE), BF16),
            pltpu.VMEM((OWN_TOKENS, WIDE), BF16),
            pltpu.VMEM((8, OWN_TOKENS, C), BF16),
            pltpu.VMEM((3, 8, 8, WIDE), F32),
            pltpu.VMEM((WIDE, C), BF16),
            pltpu.VMEM((WIDE, WIDE), BF16),
            pltpu.VMEM((C, C), BF16),
            pltpu.VMEM((2048, WIDE), BF16),
            pltpu.VMEM((2048, WIDE), BF16),
            pltpu.VMEM((OWN_TOKENS, WIDE), BF16),
            pltpu.VMEM((OWN_TOKENS, WIDE), F32),
            dma((len(sources),)),
            dma((OWN, 2)),
            dma((OWN,)),
            dma((OWN, 8)),
            dma((OWN, 8)),
            dma((OWN, 4)),
            dma((OWN, 4)),
            dma((OWN, 9)),
            dma((OWN, 9)),
            dma((7,)),
            dma((7,)),
            dma((3, 7)),
            dma((3, 7)),
            dma((2, 2)),
            dma((2, 2)),
            dma((3,)),
            dma((3,)),
            dma((3,)),
            dma((3,)),
            dma((4,)),
            dma((4,)),
        ],
        compiler_params=pltpu.CompilerParams(
            collective_id=0, has_side_effects=True, vmem_limit_bytes=58 << 20
        ),
        name="unet_level",
    )(step, *sources)


def body(
    latents,
    noise_draw,
    timesteps,
    inlet_conv,
    time_first,
    time_first_bias,
    time_second,
    time_second_bias,
    conv_first,
    conv_second,
    proj_inner,
    query_weight,
    key_weight,
    value_weight,
    attn_out,
    proj_outer,
    outlet_conv,
    first_gain,
    second_gain,
    third_gain,
    final_gain,
    layer_gain,
):
    def turned(field):
        return field[0].transpose(2, 0, 1).reshape(4, OWN_TOKENS)

    halfway = C // 2
    frequency = jnp.exp(-math.log(10000.0) * jnp.arange(halfway, dtype=F32) / halfway)
    angles = timesteps.astype(F32)[:, None] * frequency[None, :]
    wave = jnp.concatenate([jnp.cos(angles), jnp.sin(angles)], axis=1)
    vectors = (first_gain, second_gain, final_gain, layer_gain, time_second_bias)
    squares = (proj_inner, query_weight, key_weight, value_weight, attn_out, proj_outer)
    sources = [
        jnp.concatenate([turned(latents), turned(noise_draw)], axis=0),
        wave,
        time_first.T,
        time_second.T,
        conv_first.T,
        conv_second.T,
        *(m.T for m in squares),
        inlet_conv,
        outlet_conv.T,
        time_first_bias.reshape(1, 4 * C),
        *(v.reshape(1, C) for v in vectors),
        third_gain.reshape(1, C),
    ]
    result = run_block(timesteps, sources)
    return result.reshape(4, 4, ROW).transpose(1, 2, 0)[None]


def solution(mesh):
    in_specs = (
        P("batch", "space", None, None),
        P("batch", "space", None, None),
        P("batch"),
        P(),
        P(None, "batch"),
        P(),
        P(None, "batch"),
        P(),
        P(None, "batch"),
        P(None, "batch"),
        P(None, "batch"),
        P(None, "batch"),
        P(None, "batch"),
        P(None, "batch"),
        P(None, "batch"),
        P(None, "batch"),
        P(),
        P(),
        P(),
        P(),
        P(),
        P(),
    )
    out_specs = P("batch", "space", None, None)
    return jax.shard_map(body, mesh=mesh, in_specs=in_specs, out_specs=out_specs, check_vma=False)
```

```python
import math

import jax
import jax.numpy as jnp
from jax import lax
from jax.experimental import pallas as pl
from jax.experimental.pallas import tpu as pltpu
from jax.sharding import PartitionSpec as P

HEADS = 8
HEAD_SIZE = 40
GROUPS = 32
STEPS = 1000


EPS_GROUP = 1e-06
EPS_BLOCK = 1e-05
EPS_LAYER = 1e-05


C = 320
WIDE = 512
ROW = 64
OWN_TOKENS = 256
EDGED = OWN_TOKENS + 2 * ROW
TAPS = 2944
LENGTHS = (1408, 1408, 1280, 1280)
BASES = (0, 2816, 5632, 8192)
LANES = 10752
OWN = 4
AT_SECOND = 1280
AT_CONV_ONE = 2560
AT_CONV_TWO = 5504
AT_INNER, AT_QUERY, AT_KEY, AT_VALUE, AT_MIX, AT_OUTER = (8448 + 384 * i for i in range(6))
MESH = pl.DeviceIdType.MESH
F32 = jnp.float32
BF16 = jnp.bfloat16


def mm(a, b):
    return lax.dot_general(a, b, (((1,), (0,)), ((), ())), preferred_element_type=F32)


def mt(a, b):
    return lax.dot_general(a, b, (((1,), (1,)), ((), ())), preferred_element_type=F32)


def exactly(product, v, matrix):
    count = v.shape[0]
    high = v.astype(BF16).astype(F32)
    mid = (v - high).astype(BF16).astype(F32)
    low = v - high - mid
    parts = product(jnp.concatenate([high, mid, low], axis=0).astype(BF16), matrix)
    return parts[:count] + parts[count : 2 * count] + parts[2 * count :]


def silu(v):
    half = 0.5 * v
    return half + half * jnp.tanh(half)


def block_kernel(step, *refs):
    sources = refs[:21]
    out = refs[21]
    held = refs[22:43]
    (
        w0,
        w1,
        w2,
        w3,
        wn,
        flat,
        taps,
        xt,
        nt,
        nview,
        start,
        mid6,
        two6,
        block,
        nat,
        stats,
        spread,
        gwide,
        gslim,
        keys,
        values,
        query,
        base,
        l_s,
        y_s,
        y_r,
        a_s,
        a_r,
        b_s,
        b_r,
        c_s,
        c_r,
        n_s,
        n_r,
        t_s,
        t_r,
        h_s,
        h_r,
        up_s,
        up_r,
        dn_s,
        dn_r,
        k_s,
        k_r,
    ) = refs[43:]
    w = (w0, w1, w2, w3)
    b = lax.axis_index("batch")
    s = lax.axis_index("space")
    yh = lax.rem(b, 2)
    z = lax.rem(lax.div(b, 2), 8)
    x = lax.div(b, 16)
    core = lax.rem(s, 2)
    chip = lax.div(s, 2)
    sib = s + 1 - 2 * core
    mate = b + 1 - 2 * yh

    loads = [pltpu.make_async_copy(h, v, l_s.at[i]) for i, (h, v) in enumerate(zip(sources, held))]
    for load in loads:
        load.start()

    def at_z(d):
        return ((x * 8 + lax.rem(z + d, 8)) * 2 + yh, s)

    def at_x(d):
        return ((lax.rem(x + d, 4) * 8 + z) * 2 + yh, s)

    peers = [lax.rem(s + d, 8) for d in range(8)]
    barrier = pltpu.get_barrier_semaphore()
    edge = jnp.where(chip >= 2, core, 6 + core)
    friends = [(mate, edge), at_z(1), at_z(7), at_x(1), at_x(3)] + [(b, q) for q in peers[1:]]
    for dev in friends:
        pl.semaphore_signal(barrier, inc=1, device_id=dev, device_id_type=MESH)
    for load in loads:
        load.wait()
    field8, wave, first, second, conv_a, conv_b = held[:6]
    squares = held[6:12]
    inlet, outlet, bias_a = held[12:15]
    third = held[20]

    def eight(rows):
        rows = rows.astype(F32)
        return jnp.concatenate([rows, jnp.zeros((8 - rows.shape[0], rows.shape[1]), F32)], axis=0).astype(BF16)

    flat[...] = jnp.zeros((8, LANES), BF16)
    turned = first[...].astype(F32)
    for i in range(4):
        flat[:, C * i : C * i + C] = eight(turned[5 * i : 5 * i + 5])
    flat[:, AT_SECOND : AT_SECOND + 1280] = eight(second[...])
    flat[:, AT_CONV_ONE : AT_CONV_ONE + 9 * C] = eight(conv_a[...])
    flat[:, AT_CONV_TWO : AT_CONV_TWO + 9 * C] = eight(conv_b[...])
    for i in range(6):
        flat[:, AT_INNER + 384 * i : AT_INNER + 384 * i + C] = eight(squares[i][...])

    own = [pl.ds(pl.multiple_of(BASES[i] + core * LENGTHS[i], 128), LENGTHS[i]) for i in range(OWN)]
    for i in range(OWN):
        w[i][core, x, z, yh] = flat[:, own[i]]
    pl.semaphore_wait(barrier, 11 + jnp.where((chip == 0) | (chip == 3), 2, 0))

    def send(src, dst, ss, rs, dev):
        return pltpu.make_async_remote_copy(
            src_ref=src, dst_ref=dst, send_sem=ss, recv_sem=rs, device_id=dev, device_id_type=MESH
        )

    pending = []

    def go(copy):
        copy.start()
        pending.append(copy)
        return copy

    def crossing(i, k, to):
        return send(flat.at[:, own[i]], w[i].at[core, x, z, yh], y_s.at[i, k], y_r.at[i], (mate, 2 * to + core))

    for i in range(OWN):
        for k in range(2):

            @pl.when(chip == 0)
            def _(i=i, k=k):
                crossing(i, k, 3 - k).start()

            @pl.when(chip == 3)
            def _(i=i, k=k):
                crossing(i, k, k).start()

    place = lax.broadcasted_iota(jnp.int32, (8, 128), 0) * 128 + lax.broadcasted_iota(jnp.int32, (8, 128), 1)
    root = math.sqrt(0.00085) + place.astype(F32) / (STEPS - 1) * (math.sqrt(0.012) - math.sqrt(0.00085))
    abar = jnp.where(place <= step[0], 1.0 - root * root, 1.0)
    for shift in (1, 2, 4, 8, 16, 32, 64):
        abar = abar * pltpu.roll(abar, shift, 1)
    for shift in (1, 2, 4):
        abar = abar * pltpu.roll(abar, shift, 0)
    abar = abar[0:1, 0:1]
    noisy = jnp.sqrt(abar) * field8[0:4, :] + jnp.sqrt(1.0 - abar) * field8[4:8, :]
    noisy = noisy.astype(BF16).astype(F32)
    place = lax.bitwise_and(lax.broadcasted_iota(jnp.int32, (4, OWN_TOKENS), 1), ROW - 1)
    west = jnp.where(place == 0, 0.0, pltpu.roll(noisy, 1, 1))
    east = jnp.where(place == ROW - 1, 0.0, pltpu.roll(noisy, OWN_TOKENS - 1, 1))
    shifted = jnp.concatenate([west, noisy, east, jnp.zeros((4, OWN_TOKENS), F32)], axis=0).astype(BF16)
    nt[...] = shifted
    nview[s] = shifted
    ns = []
    for d in range(1, 8):
        ns.append(go(send(nt, nview.at[s], n_s.at[d - 1], n_r.at[d - 1], (b, peers[d]))))

    def z_ring(i, view, half):
        def block(d):
            return view(lax.rem(z + 8 + d, 8))

        def copies(t):
            if t < 3:
                one, two = block(-t), block(t)
            else:
                one, two = half(lax.rem(z + 8 - t, 8), 0), half(lax.rem(z + t, 8), 1)
            return (
                send(one, one, a_s.at[i, 2 * t], a_r.at[i, 2 * t], at_z(1)),
                send(two, two, a_s.at[i, 2 * t + 1], a_r.at[i, 2 * t + 1], at_z(7)),
            )

        def landed(t):
            if t < 3:
                return block(-1 - t), block(1 + t)
            return half(lax.rem(z + 4, 8), 0), half(lax.rem(z + 4, 8), 1)

        return 4, copies, landed

    def x_ring(i, view, half):
        def block(d):
            return view(lax.rem(x + 4 + d, 4))

        def copies(t):
            if t < 1:
                one, two = block(0), block(0)
            else:
                one, two = half(lax.rem(x + 3, 4), 0), half(lax.rem(x + 1, 4), 1)
            return (
                send(one, one, b_s.at[i, 2 * t], b_r.at[i, 2 * t], at_x(1)),
                send(two, two, b_s.at[i, 2 * t + 1], b_r.at[i, 2 * t + 1], at_x(3)),
            )

        def landed(t):
            if t < 1:
                return block(-1), block(1)
            return half(lax.rem(x + 2, 4), 0), half(lax.rem(x + 2, 4), 1)

        return 2, copies, landed

    def rings(i, k):
        wk = w[i].at[k]
        if i % 2 == 0:
            small = z_ring(i, lambda q: wk.at[x, q], lambda q, h: wk.at[x, q, h])
            large = x_ring(i, lambda q: wk.at[q], lambda q, h: wk.at[q, pl.ds(4 * h, 4)])
            mine = wk.at[x]
        else:
            small = x_ring(i, lambda q: wk.at[q, z], lambda q, h: wk.at[q, z, h])
            large = z_ring(i, lambda q: wk.at[:, q], lambda q, h: wk.at[pl.ds(2 * h, 2), q])
            mine = wk.at[:, z]
        return small, large, mine

    mine_rings = [rings(i, core) for i in range(OWN)]
    theirs = [rings(i, 1 - core) for i in range(OWN)]
    flying = {}

    def launch(i, which, t):
        flying[i, which, t] = [go(copy) for copy in mine_rings[i][which][1](t)]

    def to_sib(i, j, ref):
        go(send(ref, ref, c_s.at[i, j], c_r.at[i, j], (b, sib)))

    def land(i, which, t):
        count, _, landed = mine_rings[i][which]
        for copy in flying[i, which, t]:
            copy.wait_recv()
        if t + 1 < count:
            launch(i, which, t + 1)
        elif which == 0:
            launch(i, 1, 0)
            to_sib(i, 0, mine_rings[i][2])
        if which == 1:
            for j, ref in enumerate(landed(t)):
                to_sib(i, 1 + 2 * t + j, ref)

    def cross(i):
        send(flat.at[:, own[i]], w[i].at[core, x, z, 1 - yh], y_s.at[i, 0], y_r.at[i], (mate, s)).wait_recv()
        launch(i, 0, 0)

    def unpack(i):
        count, _, landed = theirs[i][1]
        refs = [theirs[i][2]] + [ref for t in range(count) for ref in landed(t)]
        for j, ref in enumerate(refs):
            send(ref, ref, c_s.at[i, j], c_r.at[i, j], (b, sib)).wait_recv()

        def two(p, _):
            for k in range(2):
                both = w[i][k, lax.div(p, 8), lax.rem(p, 8)].astype(F32).reshape(16, LENGTHS[i])
                at = BASES[i] + k * LENGTHS[i]
                wn[pl.ds(pl.multiple_of(p * 16, 16), 16), at : at + LENGTHS[i]] = both.astype(BF16)
            return 0

        lax.fori_loop(0, 32, two, 0)

    wide_i = lax.broadcasted_iota(jnp.int32, (WIDE, C), 0)
    slim_j = lax.broadcasted_iota(jnp.int32, (WIDE, C), 1)
    hit = (lax.shift_right_logical(wide_i, 3) * 5 + lax.bitwise_and(wide_i, 7) == slim_j) & (
        lax.bitwise_and(wide_i, 7) < 5
    )
    spread[...] = jnp.where(hit, 1.0, 0.0).astype(BF16)
    cross(0)
    cross(1)
    gi = lax.broadcasted_iota(jnp.int32, (WIDE, WIDE), 0)
    gj = lax.broadcasted_iota(jnp.int32, (WIDE, WIDE), 1)
    same = lax.shift_right_logical(gi, 4) == lax.shift_right_logical(gj, 4)
    gwide[...] = jnp.where(same, 1.0, 0.0).astype(BF16)
    ni = lax.broadcasted_iota(jnp.int32, (C, C), 0)
    nj = lax.broadcasted_iota(jnp.int32, (C, C), 1)
    apart = ni - lax.div(nj, 10) * 10
    gslim[...] = jnp.where((apart >= 0) & (apart < 10), 1.0, 0.0).astype(BF16)
    cross(2)
    cross(3)
    vecs = jnp.concatenate([v[...].reshape(1, C) for v in held[15:20]] + [jnp.zeros((3, C), F32)], axis=0)
    wide_vecs = exactly(mt, vecs, spread[...])
    taken = inlet[...].astype(F32)
    taken = [jnp.concatenate([taken[12 * q : 12 * q + 12], jnp.zeros((4, C), F32)], axis=0) for q in range(3)]
    win = jnp.concatenate(taken + [jnp.zeros((80, C), F32)], axis=0).astype(BF16)
    win_wide = mt(win, spread[...]).astype(BF16)
    land(1, 0, 0)
    land(0, 0, 0)
    land(3, 0, 0)
    land(2, 0, 0)

    for copy in ns:
        copy.wait_recv()
    field = jnp.concatenate([nview[q] for q in range(8)], axis=1).astype(F32)
    token = lax.broadcasted_iota(jnp.int32, (16, 2048), 1)
    above = jnp.where(token < ROW, 0.0, pltpu.roll(field, ROW, 1))
    below = jnp.where(token >= 2048 - ROW, 0.0, pltpu.roll(field, 2048 - ROW, 1))
    rows = jnp.concatenate([above, field, below, jnp.zeros((80, 2048), F32)], axis=0)
    xt[0:ROW, :] = jnp.zeros((ROW, 128), BF16)
    xt[ROW + 2048 : 2 * ROW + 2048, :] = jnp.zeros((ROW, 128), BF16)
    xt[ROW : ROW + 2048, :] = rows.T.astype(BF16)

    land(1, 0, 1)
    land(0, 0, 1)
    land(2, 0, 1)
    land(0, 0, 2)
    land(2, 0, 2)
    land(0, 0, 3)

    def start_sums(q, carry):
        total, squared = carry
        part = mm(xt[pl.ds(pl.multiple_of(ROW + q * 256, 64), 256), :], win_wide)
        part = part.astype(BF16).astype(F32)
        return total + jnp.sum(part, axis=0, keepdims=True), squared + jnp.sum(part * part, axis=0, keepdims=True)

    zero = jnp.zeros((1, WIDE), F32)
    total, squared = lax.fori_loop(0, 8, start_sums, (zero, zero))
    start[...] = mm(xt[pl.ds(pl.multiple_of(s * 256, 256), EDGED), :], win_wide).astype(BF16)

    def stacked(total, squared):
        width = total.shape[1]
        return jnp.concatenate([total, squared, jnp.zeros((6, width), F32)], axis=0)

    def affine(sums, groups, gain, epsilon):
        sums = exactly(mm, sums, groups) * (1.0 / 20480.0)
        mean = sums[0:1]
        factor = lax.rsqrt(sums[1:2] - mean * mean + epsilon) * gain
        return factor, -mean * factor

    line = lax.broadcasted_iota(jnp.int32, (EDGED, 1), 0)
    outside = ((s == 0) & (line < ROW)) | ((s == 7) & (line >= EDGED - ROW))
    column = lax.bitwise_and(line, ROW - 1)

    def into_taps(field, factor, shift):
        active = jnp.where(outside, 0.0, silu(field.astype(F32) * factor + shift)).astype(BF16)
        slim = mm(active, spread[...])
        west = jnp.where(column == 0, 0.0, pltpu.roll(slim, 1, 0)).astype(BF16)
        east = jnp.where(column == ROW - 1, 0.0, pltpu.roll(slim, EDGED - 1, 0)).astype(BF16)
        for dx, shifted in enumerate((west, slim.astype(BF16), east)):
            for dy in range(3):
                tap = 3 * dy + dx
                taps[:, tap * C : (tap + 1) * C] = shifted[dy * ROW : dy * ROW + OWN_TOKENS]

    land(1, 1, 0)
    land(3, 0, 1)
    taps[:, 9 * C :] = jnp.zeros((OWN_TOKENS, TAPS - 9 * C), BF16)
    factor, shift = affine(stacked(total, squared), gwide[...], wide_vecs[0:1], EPS_BLOCK)
    into_taps(start[...], factor, shift)

    land(1, 1, 1)
    land(3, 1, 0)
    land(0, 1, 0)
    land(2, 0, 3)
    row_p = lax.broadcasted_iota(jnp.int32, (C, 1), 0)
    target = 4 * row_p - 3 * lax.rem(row_p, 5)
    unit = lax.broadcasted_iota(jnp.int32, (C, 1280), 1)
    orders = [jnp.where(unit == target + 5 * i, 1.0, 0.0).astype(BF16) for i in range(4)]
    bias_rows = jnp.broadcast_to(bias_a[...].reshape(1, 4 * C), (8, 4 * C))
    biases = [exactly(mt, exactly(mt, bias_rows, orders[i]), spread[...]) for i in range(4)]
    land(1, 1, 2)
    land(3, 1, 1)
    land(0, 1, 1)
    unpack(0)
    land(1, 1, 3)
    unpack(1)
    waves = jnp.broadcast_to(wave[...], (8, C))
    hidden = jnp.zeros((8, 1280), F32)
    for i in range(4):
        blank = jnp.zeros((8, C), F32)
        placed = jnp.concatenate([waves, blank] if i % 2 == 0 else [blank, waves], axis=1).astype(BF16)
        first_at = 640 * (i // 2)
        inner = mt(placed, wn[:, first_at : first_at + 640])
        part = silu(silu(inner + biases[i])).astype(BF16)
        hidden = hidden + mm(mm(part, spread[...]).astype(BF16), orders[i])
    embedded = mt(hidden.astype(BF16), wn[:, AT_SECOND : AT_SECOND + 1280])[0:1] + wide_vecs[4:5]
    land(3, 1, 2)
    land(2, 1, 0)
    middle = (mt(taps[...], wn[:, AT_CONV_ONE : AT_CONV_ONE + TAPS]) + embedded).astype(BF16)

    def exchange(layer, field, edged):
        edged[ROW : ROW + OWN_TOKENS, :] = field
        wide = field.astype(F32)
        stats[layer, s] = stacked(jnp.sum(wide, axis=0, keepdims=True), jnp.sum(wide * wide, axis=0, keepdims=True))
        up = send(
            edged.at[pl.ds(ROW, ROW)],
            edged.at[pl.ds(ROW + OWN_TOKENS, ROW)],
            h_s.at[layer, 0],
            h_r.at[layer, 0],
            (b, lax.rem(s + 7, 8)),
        )
        down = send(
            edged.at[pl.ds(OWN_TOKENS, ROW)],
            edged.at[pl.ds(0, ROW)],
            h_s.at[layer, 1],
            h_r.at[layer, 1],
            (b, lax.rem(s + 1, 8)),
        )

        @pl.when(s > 0)
        def _():
            up.start()

        @pl.when(s < 7)
        def _():
            down.start()

        copies = []
        for d in range(1, 8):
            copy = send(
                stats.at[layer, s], stats.at[layer, s], t_s.at[layer, d - 1], t_r.at[layer, d - 1], (b, peers[d])
            )
            copy.start()
            copies.append(copy)
            pending.append(copy)
        return up, down, copies

    def gather_stats(layer, copies):
        for copy in copies:
            copy.wait_recv()
        sums = stats[layer, 0]
        for q in range(1, 8):
            sums = sums + stats[layer, q]
        return sums

    def exchanged(layer, up, down, copies):
        @pl.when(s < 7)
        def _():
            up.wait_recv()

        @pl.when(s > 0)
        def _():
            down.wait_recv()

        @pl.when(s > 0)
        def _():
            up.wait_send()

        @pl.when(s < 7)
        def _():
            down.wait_send()

        return gather_stats(layer, copies)

    swap = exchange(0, middle, mid6)
    land(2, 1, 1)
    unpack(2)
    land(3, 1, 3)
    sums = exchanged(0, *swap)
    factor, shift = affine(sums, gwide[...], wide_vecs[1:2], EPS_BLOCK)
    into_taps(mid6[...], factor, shift)
    unpack(3)
    one = mt(taps[...], wn[:, AT_CONV_TWO : AT_CONV_TWO + TAPS])
    one = (one + start[ROW : ROW + OWN_TOKENS, :].astype(F32)).astype(BF16)
    block[...] = one

    slim = mm(one, spread[...])
    nat[s] = slim.astype(BF16)
    slim_sums = stacked(jnp.sum(slim, axis=0, keepdims=True), jnp.sum(slim * slim, axis=0, keepdims=True))
    stats[2, s] = jnp.concatenate([slim_sums, jnp.zeros((8, WIDE - C), F32)], axis=1)
    copies = []
    for d in range(1, 8):
        copy = send(stats.at[2, s], stats.at[2, s], t_s.at[2, d - 1], t_r.at[2, d - 1], (b, peers[d]))
        copy.start()
        copies.append(copy)
        pending.append(copy)

    def hop(source, towards, ss, rs):
        return send(nat.at[source], nat.at[source], ss, rs, (b, towards))

    first_up = hop(s, lax.rem(s + 2, 8), up_s.at[0], up_r.at[0])
    first_dn = hop(s, lax.rem(s + 6, 8), dn_s.at[0], dn_r.at[0])

    @pl.when(chip < 3)
    def _():
        first_up.start()

    @pl.when(chip > 0)
    def _():
        first_dn.start()

    def coming_up(h):
        return hop(s - 2 * h, lax.rem(s + 2, 8), up_s.at[0], up_r.at[h - 1])

    def going_up(h):
        return hop(s - 2 * h, lax.rem(s + 2, 8), up_s.at[h], up_r.at[h])

    def coming_dn(h):
        return hop(s + 2 * h, lax.rem(s + 6, 8), dn_s.at[0], dn_r.at[h - 1])

    def going_dn(h):
        return hop(s + 2 * h, lax.rem(s + 6, 8), dn_s.at[h], dn_r.at[h])

    lane = lax.broadcasted_iota(jnp.int32, (1, WIDE), 1)
    real = lax.bitwise_and(lane, 7) < 5
    sums = gather_stats(2, copies)
    factor, shift = affine(sums[:, :C], gslim[...], third[...].reshape(1, C), EPS_GROUP)

    def shares(q):
        where = pl.ds(pl.multiple_of(q * 256, 256), 256)
        at = lax.div(q, 2)
        return (
            send(keys.at[where], keys.at[where], k_s.at[at], k_r.at[at], (b, sib)),
            send(values.at[where], values.at[where], k_s.at[4 + at], k_r.at[4 + at], (b, sib)),
        )

    def tokens(q):
        normed = (nat[q].astype(F32) * factor + shift).astype(BF16)
        projected = mt(normed, wn[:, AT_INNER : AT_INNER + C])
        mean = jnp.sum(projected, axis=1, keepdims=True) * (1.0 / C)
        centred = jnp.where(real, projected - mean, 0.0)
        spreadness = jnp.sum(centred * centred, axis=1, keepdims=True) * (1.0 / C)
        inside = (centred * lax.rsqrt(spreadness + EPS_LAYER) * wide_vecs[3:4]).astype(BF16)
        inside = mm(inside, spread[...]).astype(BF16)
        where = pl.ds(pl.multiple_of(q * 256, 256), 256)
        keys[where, :] = mt(inside, wn[:, AT_KEY : AT_KEY + C]).astype(BF16)
        values[where, :] = mt(inside, wn[:, AT_VALUE : AT_VALUE + C]).astype(BF16)
        for copy in shares(q):
            copy.start()
        return projected, inside

    projected, inside = tokens(s)
    base[...] = projected
    query[...] = mt(inside, wn[:, AT_QUERY : AT_QUERY + C]).astype(BF16)
    for h in range(1, 4):

        @pl.when(chip >= h)
        def _(h=h):
            coming_up(h).wait_recv()
            if h < 3:

                @pl.when(chip < 3)
                def _():
                    going_up(h).start()

        @pl.when(chip + h <= 3)
        def _(h=h):
            coming_dn(h).wait_recv()
            if h < 3:

                @pl.when(chip > 0)
                def _():
                    going_dn(h).start()

        @pl.when(chip >= h)
        def _(h=h):
            tokens(s - 2 * h)

        @pl.when(chip + h <= 3)
        def _(h=h):
            tokens(s + 2 * h)

    for q in range(4):
        for copy in shares(2 * q + 1 - core):
            copy.wait_recv()

    scale = math.log2(math.e) / math.sqrt(HEAD_SIZE)
    half = lax.broadcasted_iota(jnp.int32, (1, 128), 1) < 64

    def two_heads(p, _):
        lanes = pl.ds(pl.multiple_of(p * 128, 128), 128)
        mine = query[:, lanes]
        key_part = keys[:, lanes]
        value_part = values[:, lanes]
        results = []
        for keep in (half, jnp.logical_not(half)):
            one_query = jnp.where(keep, mine.astype(F32), 0.0).astype(BF16)
            scores = mt(one_query, key_part)
            top = jnp.max(scores, axis=1, keepdims=True)
            weights = jnp.exp2((scores - top) * scale)
            bottom = jnp.sum(weights, axis=1, keepdims=True)
            results.append(mm(weights.astype(BF16), value_part) / bottom)
        query[:, lanes] = jnp.where(half, results[0], results[1]).astype(BF16)
        return 0

    lax.fori_loop(0, 4, two_heads, 0)
    attended = mm(query[...], spread[...]).astype(BF16)
    mixture = (mt(attended, wn[:, AT_MIX : AT_MIX + C]) + base[...]).astype(BF16)
    mixture = mm(mixture, spread[...]).astype(BF16)
    outer = mt(mixture, wn[:, AT_OUTER : AT_OUTER + C])
    two = (block[...].astype(F32) + outer).astype(BF16)
    swap = exchange(1, two, two6)
    sums = exchanged(1, *swap)
    factor, shift = affine(sums, gwide[...], wide_vecs[2:3], EPS_BLOCK)
    into_taps(two6[...], factor, shift)
    taken = outlet[...].astype(F32)
    taken = jnp.concatenate([taken, jnp.zeros((4, 9 * C), F32)], axis=0)
    taken = jnp.concatenate([taken, jnp.zeros((8, TAPS - 9 * C), F32)], axis=1).astype(BF16)
    predicted = mt(taken, taps[...])
    out[...] = (1.0 - abar) * (predicted[0:4] - field8[4:8, :])
    for i in range(OWN):
        for k in range(2):

            @pl.when(chip == 0)
            def _(i=i, k=k):
                crossing(i, k, 3 - k).wait_send()

            @pl.when(chip == 3)
            def _(i=i, k=k):
                crossing(i, k, k).wait_send()


    for copy in pending:
        copy.wait_send()

    @pl.when(chip < 3)
    def _():
        first_up.wait_send()

    @pl.when(chip > 0)
    def _():
        first_dn.wait_send()

    for q in range(4):
        for copy in shares(2 * q + core):
            copy.wait_send()
    for h in range(1, 3):

        @pl.when((chip >= h) & (chip < 3))
        def _(h=h):
            going_up(h).wait_send()

        @pl.when((chip + h <= 3) & (chip > 0))
        def _(h=h):
            going_dn(h).wait_send()


def run_block(step, sources):
    dma = pltpu.SemaphoreType.DMA
    hbm = pl.BlockSpec(memory_space=pltpu.HBM)
    return pl.pallas_call(
        block_kernel,
        out_shape=jax.ShapeDtypeStruct((4, OWN_TOKENS), F32),
        in_specs=[pl.BlockSpec(memory_space=pltpu.SMEM)] + [hbm] * len(sources),
        out_specs=pl.BlockSpec(memory_space=pltpu.VMEM),
        scratch_shapes=[pltpu.VMEM(a.shape, a.dtype) for a in sources]
        + [pltpu.VMEM((2, 4, 8, 2, 8, length), BF16) for length in LENGTHS]
        + [
            pltpu.VMEM((WIDE, LANES), BF16),
            pltpu.VMEM((8, LANES), BF16),
            pltpu.VMEM((OWN_TOKENS, TAPS), BF16),
            pltpu.VMEM((2048 + 2 * ROW, 128), BF16),
            pltpu.VMEM((16, OWN_TOKENS), BF16),
            pltpu.VMEM((8, 16, OWN_TOKENS), BF16),
            pltpu.VMEM((EDGED, WIDE), BF16),
            pltpu.VMEM((EDGED, WIDE), BF16),
            pltpu.VMEM((EDGED, WIDE), BF16),
            pltpu.VMEM((OWN_TOKENS, WIDE), BF16),
            pltpu.VMEM((8, OWN_TOKENS, C), BF16),
            pltpu.VMEM((3, 8, 8, WIDE), F32),
            pltpu.VMEM((WIDE, C), BF16),
            pltpu.VMEM((WIDE, WIDE), BF16),
            pltpu.VMEM((C, C), BF16),
            pltpu.VMEM((2048, WIDE), BF16),
            pltpu.VMEM((2048, WIDE), BF16),
            pltpu.VMEM((OWN_TOKENS, WIDE), BF16),
            pltpu.VMEM((OWN_TOKENS, WIDE), F32),
            dma((len(sources),)),
            dma((OWN, 2)),
            dma((OWN,)),
            dma((OWN, 8)),
            dma((OWN, 8)),
            dma((OWN, 4)),
            dma((OWN, 4)),
            dma((OWN, 9)),
            dma((OWN, 9)),
            dma((7,)),
            dma((7,)),
            dma((3, 7)),
            dma((3, 7)),
            dma((2, 2)),
            dma((2, 2)),
            dma((3,)),
            dma((3,)),
            dma((3,)),
            dma((3,)),
            dma((8,)),
            dma((8,)),
        ],
        compiler_params=pltpu.CompilerParams(
            collective_id=0, has_side_effects=True, vmem_limit_bytes=58 << 20
        ),
        name="unet_level",
    )(step, *sources)


def body(
    latents,
    noise_draw,
    timesteps,
    inlet_conv,
    time_first,
    time_first_bias,
    time_second,
    time_second_bias,
    conv_first,
    conv_second,
    proj_inner,
    query_weight,
    key_weight,
    value_weight,
    attn_out,
    proj_outer,
    outlet_conv,
    first_gain,
    second_gain,
    third_gain,
    final_gain,
    layer_gain,
):
    def turned(field):
        return field[0].transpose(2, 0, 1).reshape(4, OWN_TOKENS)

    halfway = C // 2
    frequency = jnp.exp(-math.log(10000.0) * jnp.arange(halfway, dtype=F32) / halfway)
    angles = timesteps.astype(F32)[:, None] * frequency[None, :]
    wave = jnp.concatenate([jnp.cos(angles), jnp.sin(angles)], axis=1)
    vectors = (first_gain, second_gain, final_gain, layer_gain, time_second_bias)
    squares = (proj_inner, query_weight, key_weight, value_weight, attn_out, proj_outer)
    sources = [
        jnp.concatenate([turned(latents), turned(noise_draw)], axis=0),
        wave,
        time_first.T,
        time_second.T,
        conv_first.T,
        conv_second.T,
        *(m.T for m in squares),
        inlet_conv,
        outlet_conv.T,
        time_first_bias,
        *vectors,
        third_gain,
    ]
    result = run_block(timesteps, sources)
    return result.reshape(4, 4, ROW).transpose(1, 2, 0)[None]


def solution(mesh):
    in_specs = (
        P("batch", "space", None, None),
        P("batch", "space", None, None),
        P("batch"),
        P(),
        P(None, "batch"),
        P(),
        P(None, "batch"),
        P(),
        P(None, "batch"),
        P(None, "batch"),
        P(None, "batch"),
        P(None, "batch"),
        P(None, "batch"),
        P(None, "batch"),
        P(None, "batch"),
        P(None, "batch"),
        P(),
        P(),
        P(),
        P(),
        P(),
        P(),
    )
    out_specs = P("batch", "space", None, None)
    return jax.shard_map(body, mesh=mesh, in_specs=in_specs, out_specs=out_specs, check_vma=False)
```

```python
import math

import jax
import jax.numpy as jnp
from jax import lax
from jax.experimental import pallas as pl
from jax.experimental.pallas import tpu as pltpu
from jax.sharding import PartitionSpec as P

HEADS = 8
HEAD_SIZE = 40
GROUPS = 32
STEPS = 1000


EPS_GROUP = 1e-06
EPS_BLOCK = 1e-05
EPS_LAYER = 1e-05


C = 320
WIDE = 512
ROW = 64
OWN_TOKENS = 256
EDGED = OWN_TOKENS + 2 * ROW
TAPS = 2944
LENGTHS = (1408, 1408, 1280, 1280)
BASES = (0, 2816, 5632, 8192)
LANES = 10752
OWN = 4
AT_SECOND = 1280
AT_CONV_ONE = 2560
AT_CONV_TWO = 5504
AT_INNER, AT_QUERY, AT_KEY, AT_VALUE, AT_MIX, AT_OUTER = (8448 + 384 * i for i in range(6))
MESH = pl.DeviceIdType.MESH
F32 = jnp.float32
BF16 = jnp.bfloat16


def mm(a, b):
    return lax.dot_general(a, b, (((1,), (0,)), ((), ())), preferred_element_type=F32)


def mt(a, b):
    return lax.dot_general(a, b, (((1,), (1,)), ((), ())), preferred_element_type=F32)


def exactly(product, v, matrix):
    count = v.shape[0]
    high = v.astype(BF16).astype(F32)
    mid = (v - high).astype(BF16).astype(F32)
    low = v - high - mid
    parts = product(jnp.concatenate([high, mid, low], axis=0).astype(BF16), matrix)
    return parts[:count] + parts[count : 2 * count] + parts[2 * count :]


def silu(v):
    half = 0.5 * v
    return half + half * jnp.tanh(half)


def block_kernel(step, *refs):
    sources = refs[:21]
    out = refs[21]
    held = refs[22:43]
    (
        w0,
        w1,
        w2,
        w3,
        d0,
        d1,
        d2,
        d3,
        orders,
        pack,
        wn,
        flat,
        taps,
        xt,
        nt,
        nview,
        start,
        mid6,
        two6,
        block,
        nat,
        stats,
        spread,
        gwide,
        gslim,
        keys,
        values,
        query,
        base,
        l_s,
        y_s,
        y_r,
        a_s,
        a_r,
        b_s,
        b_r,
        c_s,
        c_r,
        n_s,
        n_r,
        t_s,
        t_r,
        h_s,
        h_r,
        up_s,
        up_r,
        dn_s,
        dn_r,
        k_s,
        k_r,
    ) = refs[43:]
    w = (w0, w1, w2, w3)
    dense = (d0, d1, d2, d3)
    b = lax.axis_index("batch")
    s = lax.axis_index("space")
    yh = lax.rem(b, 2)
    z = lax.rem(lax.div(b, 2), 8)
    x = lax.div(b, 16)
    core = lax.rem(s, 2)
    chip = lax.div(s, 2)
    sib = s + 1 - 2 * core
    mate = b + 1 - 2 * yh

    loads = [pltpu.make_async_copy(h, v, l_s.at[i]) for i, (h, v) in enumerate(zip(sources, held))]
    for load in loads:
        load.start()

    def at_z(d):
        return ((x * 8 + lax.rem(z + d, 8)) * 2 + yh, s)

    def at_x(d):
        return ((lax.rem(x + d, 4) * 8 + z) * 2 + yh, s)

    peers = [lax.rem(s + d, 8) for d in range(8)]
    barrier = pltpu.get_barrier_semaphore()
    edge = jnp.where(chip >= 2, core, 6 + core)
    friends = [(mate, edge), at_z(1), at_z(7), at_x(1), at_x(3)] + [(b, q) for q in peers[1:]]
    for dev in friends:
        pl.semaphore_signal(barrier, inc=1, device_id=dev, device_id_type=MESH)
    for load in loads:
        load.wait()
    field8, wave, first, second, conv_a, conv_b = held[:6]
    squares = held[6:12]
    inlet, outlet, bias_a = held[12:15]
    third = held[20]

    def eight(rows):
        rows = rows.astype(F32)
        return jnp.concatenate([rows, jnp.zeros((8 - rows.shape[0], rows.shape[1]), F32)], axis=0).astype(BF16)

    flat[...] = jnp.zeros((8, LANES), BF16)
    turned = first[...].astype(F32)
    for i in range(4):
        flat[:, C * i : C * i + C] = eight(turned[5 * i : 5 * i + 5])
    flat[:, AT_SECOND : AT_SECOND + 1280] = eight(second[...])
    flat[:, AT_CONV_ONE : AT_CONV_ONE + 9 * C] = eight(conv_a[...])
    flat[:, AT_CONV_TWO : AT_CONV_TWO + 9 * C] = eight(conv_b[...])
    for i in range(6):
        flat[:, AT_INNER + 384 * i : AT_INNER + 384 * i + C] = eight(squares[i][...])

    own = [pl.ds(pl.multiple_of(BASES[i] + core * LENGTHS[i], 128), LENGTHS[i]) for i in range(OWN)]
    for i in range(OWN):
        w[i][core, x, z, yh] = flat[:, own[i]]
    place = lax.broadcasted_iota(jnp.int32, (8, 128), 0) * 128 + lax.broadcasted_iota(jnp.int32, (8, 128), 1)
    root = math.sqrt(0.00085) + place.astype(F32) / (STEPS - 1) * (math.sqrt(0.012) - math.sqrt(0.00085))
    abar = jnp.where(place <= step[0], 1.0 - root * root, 1.0)
    for shift in (1, 2, 4, 8, 16, 32, 64):
        abar = abar * pltpu.roll(abar, shift, 1)
    for shift in (1, 2, 4):
        abar = abar * pltpu.roll(abar, shift, 0)
    abar = abar[0:1, 0:1]
    noisy = jnp.sqrt(abar) * field8[0:4, :] + jnp.sqrt(1.0 - abar) * field8[4:8, :]
    noisy = noisy.astype(BF16).astype(F32)
    place = lax.bitwise_and(lax.broadcasted_iota(jnp.int32, (4, OWN_TOKENS), 1), ROW - 1)
    west = jnp.where(place == 0, 0.0, pltpu.roll(noisy, 1, 1))
    east = jnp.where(place == ROW - 1, 0.0, pltpu.roll(noisy, OWN_TOKENS - 1, 1))
    shifted = jnp.concatenate([west, noisy, east, jnp.zeros((4, OWN_TOKENS), F32)], axis=0).astype(BF16)
    nt[...] = shifted
    nview[s] = shifted
    wide_i = lax.broadcasted_iota(jnp.int32, (WIDE, C), 0)
    slim_j = lax.broadcasted_iota(jnp.int32, (WIDE, C), 1)
    hit = (lax.shift_right_logical(wide_i, 3) * 5 + lax.bitwise_and(wide_i, 7) == slim_j) & (
        lax.bitwise_and(wide_i, 7) < 5
    )
    spread[...] = jnp.where(hit, 1.0, 0.0).astype(BF16)
    gi = lax.broadcasted_iota(jnp.int32, (WIDE, WIDE), 0)
    gj = lax.broadcasted_iota(jnp.int32, (WIDE, WIDE), 1)
    same = lax.shift_right_logical(gi, 4) == lax.shift_right_logical(gj, 4)
    gwide[...] = jnp.where(same, 1.0, 0.0).astype(BF16)
    ni = lax.broadcasted_iota(jnp.int32, (C, C), 0)
    nj = lax.broadcasted_iota(jnp.int32, (C, C), 1)
    apart = ni - lax.div(nj, 10) * 10
    gslim[...] = jnp.where((apart >= 0) & (apart < 10), 1.0, 0.0).astype(BF16)
    pr = lax.broadcasted_iota(jnp.int32, (80, 128), 0)
    pc = lax.broadcasted_iota(jnp.int32, (80, 128), 1)
    hit = (lax.shift_right_logical(pc, 3) * 5 + lax.bitwise_and(pc, 7) == pr) & (lax.bitwise_and(pc, 7) < 5)
    pack[...] = jnp.where(hit, 1.0, 0.0).astype(BF16)
    vecs = jnp.concatenate([v[...].reshape(1, C) for v in held[15:20]] + [jnp.zeros((3, C), F32)], axis=0)
    wide_vecs = exactly(mt, vecs, spread[...])
    taken = inlet[...].astype(F32)
    taken = [jnp.concatenate([taken[12 * q : 12 * q + 12], jnp.zeros((4, C), F32)], axis=0) for q in range(3)]
    win = jnp.concatenate(taken + [jnp.zeros((80, C), F32)], axis=0).astype(BF16)
    win_wide = mt(win, spread[...]).astype(BF16)
    row_p = lax.broadcasted_iota(jnp.int32, (C, 1), 0)
    target = 4 * row_p - 3 * lax.rem(row_p, 5)
    unit = lax.broadcasted_iota(jnp.int32, (C, 1280), 1)
    for i in range(4):
        orders[i] = jnp.where(unit == target + 5 * i, 1.0, 0.0).astype(BF16)
    bias_rows = jnp.broadcast_to(bias_a[...].reshape(1, 4 * C), (8, 4 * C))
    biases = [exactly(mt, exactly(mt, bias_rows, orders[i]), spread[...]) for i in range(4)]
    pl.semaphore_wait(barrier, 11 + jnp.where((chip == 0) | (chip == 3), 2, 0))

    def send(src, dst, ss, rs, dev):
        return pltpu.make_async_remote_copy(
            src_ref=src, dst_ref=dst, send_sem=ss, recv_sem=rs, device_id=dev, device_id_type=MESH
        )

    pending = []

    def go(copy):
        copy.start()
        pending.append(copy)
        return copy

    def crossing(i, k, to):
        return send(flat.at[:, own[i]], w[i].at[core, x, z, yh], y_s.at[i, k], y_r.at[i], (mate, 2 * to + core))

    for i in range(OWN):
        for k in range(2):

            @pl.when(chip == 0)
            def _(i=i, k=k):
                crossing(i, k, 3 - k).start()

            @pl.when(chip == 3)
            def _(i=i, k=k):
                crossing(i, k, k).start()

    ns = []
    for d in range(1, 8):
        ns.append(go(send(nt, nview.at[s], n_s.at[d - 1], n_r.at[d - 1], (b, peers[d]))))

    def z_ring(i, view, half):
        def block(d):
            return view(lax.rem(z + 8 + d, 8))

        def copies(t):
            if t < 3:
                one, two = block(-t), block(t)
            else:
                one, two = half(lax.rem(z + 8 - t, 8), 0), half(lax.rem(z + t, 8), 1)
            return (
                send(one, one, a_s.at[i, 2 * t], a_r.at[i, 2 * t], at_z(1)),
                send(two, two, a_s.at[i, 2 * t + 1], a_r.at[i, 2 * t + 1], at_z(7)),
            )

        def landed(t):
            if t < 3:
                return block(-1 - t), block(1 + t)
            return half(lax.rem(z + 4, 8), 0), half(lax.rem(z + 4, 8), 1)

        return 4, copies, landed

    def x_ring(i, view, half):
        def block(d):
            return view(lax.rem(x + 4 + d, 4))

        def copies(t):
            if t < 1:
                one, two = block(0), block(0)
            else:
                one, two = half(lax.rem(x + 3, 4), 0), half(lax.rem(x + 1, 4), 1)
            return (
                send(one, one, b_s.at[i, 2 * t], b_r.at[i, 2 * t], at_x(1)),
                send(two, two, b_s.at[i, 2 * t + 1], b_r.at[i, 2 * t + 1], at_x(3)),
            )

        def landed(t):
            if t < 1:
                return block(-1), block(1)
            return half(lax.rem(x + 2, 4), 0), half(lax.rem(x + 2, 4), 1)

        return 2, copies, landed

    def rings(i, k):
        wk = w[i].at[k]
        dk = dense[i].at[k]
        cuts = (pl.ds(0, 640), pl.ds(640, LENGTHS[i] - 640))
        if i % 2 == 0:
            small = z_ring(i, lambda q: wk.at[x, q], lambda q, h: wk.at[x, q, h])
            large = x_ring(i, lambda q: dk.at[q], lambda q, h: dk.at[q, :, cuts[h]])
            mine = dk.at[x]
        else:
            small = x_ring(i, lambda q: wk.at[q, z], lambda q, h: wk.at[q, z, h])
            large = z_ring(i, lambda q: dk.at[q], lambda q, h: dk.at[q, :, cuts[h]])
            mine = dk.at[z]
        return small, large, mine

    mine_rings = [rings(i, core) for i in range(OWN)]
    theirs = [rings(i, 1 - core) for i in range(OWN)]
    flying = {}

    def launch(i, which, t):
        flying[i, which, t] = [go(copy) for copy in mine_rings[i][which][1](t)]

    def to_sib(i, j, ref):
        go(send(ref, ref, c_s.at[i, j], c_r.at[i, j], (b, sib)))

    def land(i, which, t):
        count, _, landed = mine_rings[i][which]
        for copy in flying[i, which, t]:
            copy.wait_recv()
        if t + 1 < count:
            launch(i, which, t + 1)
        elif which == 0:
            if i % 2 == 0:
                rows = w[i][core, x].astype(F32).reshape(128, LENGTHS[i]).astype(BF16)
                dense[i][core, x] = mm(pack[...], rows).astype(BF16)
            else:
                rows = w[i][core, :, z].astype(F32).reshape(64, LENGTHS[i]).astype(BF16)
                dense[i][core, z] = mm(pack[0:40, 0:64], rows).astype(BF16)
            launch(i, 1, 0)
            to_sib(i, 0, mine_rings[i][2])
        if which == 1:
            for j, ref in enumerate(landed(t)):
                to_sib(i, 1 + 2 * t + j, ref)

    def cross(i):
        send(flat.at[:, own[i]], w[i].at[core, x, z, 1 - yh], y_s.at[i, 0], y_r.at[i], (mate, s)).wait_recv()
        launch(i, 0, 0)

    def unpack(i):
        count, _, landed = theirs[i][1]
        refs = [theirs[i][2]] + [ref for t in range(count) for ref in landed(t)]
        for j, ref in enumerate(refs):
            send(ref, ref, c_s.at[i, j], c_r.at[i, j], (b, sib)).wait_recv()

        grow = pack[...].astype(F32).T.astype(BF16)

        def wide_rows(q, _):
            for k in range(2):
                at = BASES[i] + k * LENGTHS[i]
                lanes = slice(at, at + LENGTHS[i])
                if i % 2 == 0:
                    rows = mm(grow, dense[i][k, q]).astype(BF16)
                    wn[pl.ds(pl.multiple_of(q * 128, 128), 128), lanes] = rows
                else:
                    rows = mm(grow[0:64, 0:40], dense[i][k, q]).astype(BF16)
                    for xx in range(4):
                        wn[pl.ds(pl.multiple_of(128 * xx + q * 16, 16), 16), lanes] = rows[16 * xx : 16 * xx + 16]
            return 0

        lax.fori_loop(0, 8 if i % 2 else 4, wide_rows, 0)

    cross(0)
    cross(1)
    cross(2)
    cross(3)
    land(1, 0, 0)
    land(0, 0, 0)
    land(3, 0, 0)
    land(2, 0, 0)

    for copy in ns:
        copy.wait_recv()
    field = jnp.concatenate([nview[q] for q in range(8)], axis=1).astype(F32)
    token = lax.broadcasted_iota(jnp.int32, (16, 2048), 1)
    above = jnp.where(token < ROW, 0.0, pltpu.roll(field, ROW, 1))
    below = jnp.where(token >= 2048 - ROW, 0.0, pltpu.roll(field, 2048 - ROW, 1))
    rows = jnp.concatenate([above, field, below, jnp.zeros((80, 2048), F32)], axis=0)
    xt[0:ROW, :] = jnp.zeros((ROW, 128), BF16)
    xt[ROW + 2048 : 2 * ROW + 2048, :] = jnp.zeros((ROW, 128), BF16)
    xt[ROW : ROW + 2048, :] = rows.T.astype(BF16)

    land(1, 0, 1)
    land(0, 0, 1)
    land(2, 0, 1)
    land(0, 0, 2)
    land(2, 0, 2)
    land(0, 0, 3)

    def start_sums(q, carry):
        total, squared = carry
        part = mm(xt[pl.ds(pl.multiple_of(ROW + q * 256, 64), 256), :], win_wide)
        part = part.astype(BF16).astype(F32)
        return total + jnp.sum(part, axis=0, keepdims=True), squared + jnp.sum(part * part, axis=0, keepdims=True)

    zero = jnp.zeros((1, WIDE), F32)
    total, squared = lax.fori_loop(0, 8, start_sums, (zero, zero))
    start[...] = mm(xt[pl.ds(pl.multiple_of(s * 256, 256), EDGED), :], win_wide).astype(BF16)

    def stacked(total, squared):
        width = total.shape[1]
        return jnp.concatenate([total, squared, jnp.zeros((6, width), F32)], axis=0)

    def affine(sums, groups, gain, epsilon):
        sums = exactly(mm, sums, groups) * (1.0 / 20480.0)
        mean = sums[0:1]
        factor = lax.rsqrt(sums[1:2] - mean * mean + epsilon) * gain
        return factor, -mean * factor

    line = lax.broadcasted_iota(jnp.int32, (EDGED, 1), 0)
    outside = ((s == 0) & (line < ROW)) | ((s == 7) & (line >= EDGED - ROW))
    column = lax.bitwise_and(line, ROW - 1)

    def into_taps(field, factor, shift):
        active = jnp.where(outside, 0.0, silu(field.astype(F32) * factor + shift)).astype(BF16)
        slim = mm(active, spread[...])
        west = jnp.where(column == 0, 0.0, pltpu.roll(slim, 1, 0)).astype(BF16)
        east = jnp.where(column == ROW - 1, 0.0, pltpu.roll(slim, EDGED - 1, 0)).astype(BF16)
        for dx, shifted in enumerate((west, slim.astype(BF16), east)):
            for dy in range(3):
                tap = 3 * dy + dx
                taps[:, tap * C : (tap + 1) * C] = shifted[dy * ROW : dy * ROW + OWN_TOKENS]

    land(1, 1, 0)
    land(3, 0, 1)
    taps[:, 9 * C :] = jnp.zeros((OWN_TOKENS, TAPS - 9 * C), BF16)
    factor, shift = affine(stacked(total, squared), gwide[...], wide_vecs[0:1], EPS_BLOCK)
    into_taps(start[...], factor, shift)

    land(1, 1, 1)
    land(3, 1, 0)
    land(0, 1, 0)
    land(2, 0, 3)
    land(1, 1, 2)
    land(3, 1, 1)
    land(0, 1, 1)
    unpack(0)
    waves = jnp.broadcast_to(wave[...], (8, C))
    hidden = jnp.zeros((8, 1280), F32)
    for i in range(4):
        blank = jnp.zeros((8, C), F32)
        placed = jnp.concatenate([waves, blank] if i % 2 == 0 else [blank, waves], axis=1).astype(BF16)
        first_at = 640 * (i // 2)
        inner = mt(placed, wn[:, first_at : first_at + 640])
        part = silu(silu(inner + biases[i])).astype(BF16)
        hidden = hidden + mm(mm(part, spread[...]).astype(BF16), orders[i])
    embedded = mt(hidden.astype(BF16), wn[:, AT_SECOND : AT_SECOND + 1280])[0:1] + wide_vecs[4:5]
    land(1, 1, 3)
    unpack(1)
    land(3, 1, 2)
    land(2, 1, 0)
    middle = (mt(taps[...], wn[:, AT_CONV_ONE : AT_CONV_ONE + TAPS]) + embedded).astype(BF16)

    def exchange(layer, field, edged):
        edged[ROW : ROW + OWN_TOKENS, :] = field
        wide = field.astype(F32)
        stats[layer, s] = stacked(jnp.sum(wide, axis=0, keepdims=True), jnp.sum(wide * wide, axis=0, keepdims=True))
        up = send(
            edged.at[pl.ds(ROW, ROW)],
            edged.at[pl.ds(ROW + OWN_TOKENS, ROW)],
            h_s.at[layer, 0],
            h_r.at[layer, 0],
            (b, lax.rem(s + 7, 8)),
        )
        down = send(
            edged.at[pl.ds(OWN_TOKENS, ROW)],
            edged.at[pl.ds(0, ROW)],
            h_s.at[layer, 1],
            h_r.at[layer, 1],
            (b, lax.rem(s + 1, 8)),
        )

        @pl.when(s > 0)
        def _():
            up.start()

        @pl.when(s < 7)
        def _():
            down.start()

        copies = []
        for d in range(1, 8):
            copy = send(
                stats.at[layer, s], stats.at[layer, s], t_s.at[layer, d - 1], t_r.at[layer, d - 1], (b, peers[d])
            )
            copy.start()
            copies.append(copy)
            pending.append(copy)
        return up, down, copies

    def gather_stats(layer, copies):
        for copy in copies:
            copy.wait_recv()
        sums = stats[layer, 0]
        for q in range(1, 8):
            sums = sums + stats[layer, q]
        return sums

    def exchanged(layer, up, down, copies):
        @pl.when(s < 7)
        def _():
            up.wait_recv()

        @pl.when(s > 0)
        def _():
            down.wait_recv()

        @pl.when(s > 0)
        def _():
            up.wait_send()

        @pl.when(s < 7)
        def _():
            down.wait_send()

        return gather_stats(layer, copies)

    swap = exchange(0, middle, mid6)
    land(2, 1, 1)
    unpack(2)
    land(3, 1, 3)
    sums = exchanged(0, *swap)
    factor, shift = affine(sums, gwide[...], wide_vecs[1:2], EPS_BLOCK)
    into_taps(mid6[...], factor, shift)
    unpack(3)
    one = mt(taps[...], wn[:, AT_CONV_TWO : AT_CONV_TWO + TAPS])
    one = (one + start[ROW : ROW + OWN_TOKENS, :].astype(F32)).astype(BF16)
    block[...] = one

    slim = mm(one, spread[...])
    nat[s] = slim.astype(BF16)
    slim_sums = stacked(jnp.sum(slim, axis=0, keepdims=True), jnp.sum(slim * slim, axis=0, keepdims=True))
    stats[2, s] = jnp.concatenate([slim_sums, jnp.zeros((8, WIDE - C), F32)], axis=1)
    copies = []
    for d in range(1, 8):
        copy = send(stats.at[2, s], stats.at[2, s], t_s.at[2, d - 1], t_r.at[2, d - 1], (b, peers[d]))
        copy.start()
        copies.append(copy)
        pending.append(copy)

    def hop(source, towards, ss, rs):
        return send(nat.at[source], nat.at[source], ss, rs, (b, towards))

    first_up = hop(s, lax.rem(s + 2, 8), up_s.at[0], up_r.at[0])
    first_dn = hop(s, lax.rem(s + 6, 8), dn_s.at[0], dn_r.at[0])

    @pl.when(chip < 3)
    def _():
        first_up.start()

    @pl.when(chip > 0)
    def _():
        first_dn.start()

    def coming_up(h):
        return hop(s - 2 * h, lax.rem(s + 2, 8), up_s.at[0], up_r.at[h - 1])

    def going_up(h):
        return hop(s - 2 * h, lax.rem(s + 2, 8), up_s.at[h], up_r.at[h])

    def coming_dn(h):
        return hop(s + 2 * h, lax.rem(s + 6, 8), dn_s.at[0], dn_r.at[h - 1])

    def going_dn(h):
        return hop(s + 2 * h, lax.rem(s + 6, 8), dn_s.at[h], dn_r.at[h])

    lane = lax.broadcasted_iota(jnp.int32, (1, WIDE), 1)
    real = lax.bitwise_and(lane, 7) < 5
    sums = gather_stats(2, copies)
    factor, shift = affine(sums[:, :C], gslim[...], third[...].reshape(1, C), EPS_GROUP)

    def shares(q):
        where = pl.ds(pl.multiple_of(q * 256, 256), 256)
        at = lax.div(q, 2)
        return (
            send(keys.at[where], keys.at[where], k_s.at[at], k_r.at[at], (b, sib)),
            send(values.at[where], values.at[where], k_s.at[4 + at], k_r.at[4 + at], (b, sib)),
        )

    def tokens(q):
        normed = (nat[q].astype(F32) * factor + shift).astype(BF16)
        projected = mt(normed, wn[:, AT_INNER : AT_INNER + C])
        mean = jnp.sum(projected, axis=1, keepdims=True) * (1.0 / C)
        centred = jnp.where(real, projected - mean, 0.0)
        spreadness = jnp.sum(centred * centred, axis=1, keepdims=True) * (1.0 / C)
        inside = (centred * lax.rsqrt(spreadness + EPS_LAYER) * wide_vecs[3:4]).astype(BF16)
        inside = mm(inside, spread[...]).astype(BF16)
        where = pl.ds(pl.multiple_of(q * 256, 256), 256)
        keys[where, :] = mt(inside, wn[:, AT_KEY : AT_KEY + C]).astype(BF16)
        values[where, :] = mt(inside, wn[:, AT_VALUE : AT_VALUE + C]).astype(BF16)
        for copy in shares(q):
            copy.start()
        return projected, inside

    projected, inside = tokens(s)
    base[...] = projected
    query[...] = mt(inside, wn[:, AT_QUERY : AT_QUERY + C]).astype(BF16)
    for h in range(1, 4):

        @pl.when(chip >= h)
        def _(h=h):
            coming_up(h).wait_recv()
            if h < 3:

                @pl.when(chip < 3)
                def _():
                    going_up(h).start()

        @pl.when(chip + h <= 3)
        def _(h=h):
            coming_dn(h).wait_recv()
            if h < 3:

                @pl.when(chip > 0)
                def _():
                    going_dn(h).start()

        @pl.when(chip >= h)
        def _(h=h):
            tokens(s - 2 * h)

        @pl.when(chip + h <= 3)
        def _(h=h):
            tokens(s + 2 * h)

    for q in range(4):
        for copy in shares(2 * q + 1 - core):
            copy.wait_recv()

    scale = math.log2(math.e) / math.sqrt(HEAD_SIZE)
    half = lax.broadcasted_iota(jnp.int32, (1, 128), 1) < 64

    def two_heads(p, _):
        lanes = pl.ds(pl.multiple_of(p * 128, 128), 128)
        mine = query[:, lanes]
        key_part = keys[:, lanes]
        value_part = values[:, lanes]
        results = []
        for keep in (half, jnp.logical_not(half)):
            one_query = jnp.where(keep, mine.astype(F32), 0.0).astype(BF16)
            scores = mt(one_query, key_part)
            top = jnp.max(scores, axis=1, keepdims=True)
            weights = jnp.exp2((scores - top) * scale)
            bottom = jnp.sum(weights, axis=1, keepdims=True)
            results.append(mm(weights.astype(BF16), value_part) / bottom)
        query[:, lanes] = jnp.where(half, results[0], results[1]).astype(BF16)
        return 0

    lax.fori_loop(0, 4, two_heads, 0)
    attended = mm(query[...], spread[...]).astype(BF16)
    mixture = (mt(attended, wn[:, AT_MIX : AT_MIX + C]) + base[...]).astype(BF16)
    mixture = mm(mixture, spread[...]).astype(BF16)
    outer = mt(mixture, wn[:, AT_OUTER : AT_OUTER + C])
    two = (block[...].astype(F32) + outer).astype(BF16)
    swap = exchange(1, two, two6)
    sums = exchanged(1, *swap)
    factor, shift = affine(sums, gwide[...], wide_vecs[2:3], EPS_BLOCK)
    into_taps(two6[...], factor, shift)
    taken = outlet[...].astype(F32)
    taken = jnp.concatenate([taken, jnp.zeros((4, 9 * C), F32)], axis=0)
    taken = jnp.concatenate([taken, jnp.zeros((8, TAPS - 9 * C), F32)], axis=1).astype(BF16)
    predicted = mt(taken, taps[...])
    out[...] = (1.0 - abar) * (predicted[0:4] - field8[4:8, :])
    for i in range(OWN):
        for k in range(2):

            @pl.when(chip == 0)
            def _(i=i, k=k):
                crossing(i, k, 3 - k).wait_send()

            @pl.when(chip == 3)
            def _(i=i, k=k):
                crossing(i, k, k).wait_send()


    for copy in pending:
        copy.wait_send()

    @pl.when(chip < 3)
    def _():
        first_up.wait_send()

    @pl.when(chip > 0)
    def _():
        first_dn.wait_send()

    for q in range(4):
        for copy in shares(2 * q + core):
            copy.wait_send()
    for h in range(1, 3):

        @pl.when((chip >= h) & (chip < 3))
        def _(h=h):
            going_up(h).wait_send()

        @pl.when((chip + h <= 3) & (chip > 0))
        def _(h=h):
            going_dn(h).wait_send()


def run_block(step, sources):
    dma = pltpu.SemaphoreType.DMA
    hbm = pl.BlockSpec(memory_space=pltpu.HBM)
    return pl.pallas_call(
        block_kernel,
        out_shape=jax.ShapeDtypeStruct((4, OWN_TOKENS), F32),
        in_specs=[pl.BlockSpec(memory_space=pltpu.SMEM)] + [hbm] * len(sources),
        out_specs=pl.BlockSpec(memory_space=pltpu.VMEM),
        scratch_shapes=[pltpu.VMEM(a.shape, a.dtype) for a in sources]
        + [pltpu.VMEM((2, 4, 8, 2, 8, length), BF16) for length in LENGTHS]
        + [pltpu.VMEM((2, 8, 40, n) if i % 2 else (2, 4, 80, n), BF16) for i, n in enumerate(LENGTHS)]
        + [pltpu.VMEM((4, C, 4 * C), BF16), pltpu.VMEM((80, 128), BF16)]
        + [
            pltpu.VMEM((WIDE, LANES), BF16),
            pltpu.VMEM((8, LANES), BF16),
            pltpu.VMEM((OWN_TOKENS, TAPS), BF16),
            pltpu.VMEM((2048 + 2 * ROW, 128), BF16),
            pltpu.VMEM((16, OWN_TOKENS), BF16),
            pltpu.VMEM((8, 16, OWN_TOKENS), BF16),
            pltpu.VMEM((EDGED, WIDE), BF16),
            pltpu.VMEM((EDGED, WIDE), BF16),
            pltpu.VMEM((EDGED, WIDE), BF16),
            pltpu.VMEM((OWN_TOKENS, WIDE), BF16),
            pltpu.VMEM((8, OWN_TOKENS, C), BF16),
            pltpu.VMEM((3, 8, 8, WIDE), F32),
            pltpu.VMEM((WIDE, C), BF16),
            pltpu.VMEM((WIDE, WIDE), BF16),
            pltpu.VMEM((C, C), BF16),
            pltpu.VMEM((2048, WIDE), BF16),
            pltpu.VMEM((2048, WIDE), BF16),
            pltpu.VMEM((OWN_TOKENS, WIDE), BF16),
            pltpu.VMEM((OWN_TOKENS, WIDE), F32),
            dma((len(sources),)),
            dma((OWN, 2)),
            dma((OWN,)),
            dma((OWN, 8)),
            dma((OWN, 8)),
            dma((OWN, 4)),
            dma((OWN, 4)),
            dma((OWN, 9)),
            dma((OWN, 9)),
            dma((7,)),
            dma((7,)),
            dma((3, 7)),
            dma((3, 7)),
            dma((2, 2)),
            dma((2, 2)),
            dma((3,)),
            dma((3,)),
            dma((3,)),
            dma((3,)),
            dma((8,)),
            dma((8,)),
        ],
        compiler_params=pltpu.CompilerParams(
            collective_id=0, has_side_effects=True, vmem_limit_bytes=58 << 20
        ),
        name="unet_level",
    )(step, *sources)


def body(
    latents,
    noise_draw,
    timesteps,
    inlet_conv,
    time_first,
    time_first_bias,
    time_second,
    time_second_bias,
    conv_first,
    conv_second,
    proj_inner,
    query_weight,
    key_weight,
    value_weight,
    attn_out,
    proj_outer,
    outlet_conv,
    first_gain,
    second_gain,
    third_gain,
    final_gain,
    layer_gain,
):
    def turned(field):
        return field[0].transpose(2, 0, 1).reshape(4, OWN_TOKENS)

    halfway = C // 2
    frequency = jnp.exp(-math.log(10000.0) * jnp.arange(halfway, dtype=F32) / halfway)
    angles = timesteps.astype(F32)[:, None] * frequency[None, :]
    wave = jnp.concatenate([jnp.cos(angles), jnp.sin(angles)], axis=1)
    vectors = (first_gain, second_gain, final_gain, layer_gain, time_second_bias)
    squares = (proj_inner, query_weight, key_weight, value_weight, attn_out, proj_outer)
    sources = [
        jnp.concatenate([turned(latents), turned(noise_draw)], axis=0),
        wave,
        time_first.T,
        time_second.T,
        conv_first.T,
        conv_second.T,
        *(m.T for m in squares),
        inlet_conv,
        outlet_conv.T,
        time_first_bias,
        *vectors,
        third_gain,
    ]
    result = run_block(timesteps, sources)
    return result.reshape(4, 4, ROW).transpose(1, 2, 0)[None]


def solution(mesh):
    in_specs = (
        P("batch", "space", None, None),
        P("batch", "space", None, None),
        P("batch"),
        P(),
        P(None, "batch"),
        P(),
        P(None, "batch"),
        P(),
        P(None, "batch"),
        P(None, "batch"),
        P(None, "batch"),
        P(None, "batch"),
        P(None, "batch"),
        P(None, "batch"),
        P(None, "batch"),
        P(None, "batch"),
        P(),
        P(),
        P(),
        P(),
        P(),
        P(),
    )
    out_specs = P("batch", "space", None, None)
    return jax.shard_map(body, mesh=mesh, in_specs=in_specs, out_specs=out_specs, check_vma=False)
```
